32 devices in a mesh: chain: 4 (over x, core), quad: 8 (over z, y).
Axes of the slice: x: 2, y: 2, z: 4, core: 2. Of those that a mesh axis runs over, the one named last changes fastest.
Arguments:
- sections: bfloat16 [4, 4096, 4096], P('chain', 'quad'), may hold values from -8 to 8
- anchor: bfloat16 [4096, 4096], P('quad'), may hold values from -8 to 8
Outputs:
- registered: bfloat16 [4, 4096, 4096], P('chain', 'quad')
- accumulated: float32 [4, 64, 128], P('chain')
The draws below stay inside these ranges and needn't reach their ends.
All inputs are finite; a program needn't handle non-finite values.
Results may differ from the reference program's by a relative error of at most 0.00135.
The reference program's roundings to bfloat16 on the way count: a program that leaves them out, or rounds other values in their place, can miss the bound.
Values may be sent and summed in bfloat16 or wider, within the bound.
A program may use at most 128 MiB of HBM per device.

```python
import math
import jax
import jax.numpy as jnp
from jax import lax

GRID_SIZE = 64
ITERATIONS = 4
HEIGHT = 4096
COLUMNS = 4096
SLICES = 4


def box_blur(values, window, which_axis):
    lead_pad = window // 2 + 1
    tail_pad = window - 1 - window // 2
    pad_spec = [(0, 0), (0, 0)]
    pad_spec[which_axis] = (lead_pad, tail_pad)
    padded = jnp.pad(values, pad_spec, mode='wrap')
    running = jnp.cumsum(padded, axis=which_axis)
    length = values.shape[which_axis]
    upper_sums = lax.slice_in_dim(running, window, window + length, axis=which_axis)
    lower_sums = lax.slice_in_dim(running, 0, length, axis=which_axis)
    return (upper_sums - lower_sums) / window


def mode_table(point_count, mode_count):
    positions = (jnp.arange(point_count, dtype=jnp.float32) + 0.5) / point_count
    orders = jnp.arange(mode_count, dtype=jnp.float32)
    return jnp.cos(math.pi * positions[:, None] * orders[None, :])


def stack_helper(key):
    base_key = jax.random.fold_in(key, 4111)
    key_list = jax.random.split(base_key, 4)
    row_spread, col_spread, floor_gain, background, noise_level, sway_scale = (3.0, 1.5, 0.5, 0.3, 0.25, 0.3)
    texture = jax.random.normal(key_list[0], (HEIGHT, COLUMNS), jnp.float32)
    for which_axis in (0, 1):
        texture = box_blur(box_blur(texture, 3, which_axis), 3, which_axis)
    texture = texture - jnp.mean(texture)
    texture = texture / jnp.sqrt(jnp.mean(texture * texture))
    row_pos = (jnp.arange(HEIGHT, dtype=jnp.float32) + 0.5) / HEIGHT
    col_pos = (jnp.arange(COLUMNS, dtype=jnp.float32) + 0.5) / COLUMNS
    gain_field = floor_gain * jnp.exp(math.log(row_spread) * row_pos[:, None] + math.log(col_spread) * col_pos[None, :])
    row_modes = mode_table(HEIGHT, 4)
    col_modes = mode_table(COLUMNS, 4)
    steps_xy = sway_scale * jax.random.normal(key_list[1], (SLICES + 1, 2, 4, 4), jnp.float32)
    totals = jnp.cumsum(steps_xy, axis=0)
    stains = jnp.exp(jax.random.uniform(key_list[2], (SLICES + 1,), jnp.float32, -0.25, 0.25))
    flat_texture = texture.reshape(-1)
    row_coord = jnp.arange(HEIGHT, dtype=jnp.float32)[:, None]
    col_coord = jnp.arange(COLUMNS, dtype=jnp.float32)[None, :]

    def one_slice(slice_number):
        mixing = totals[slice_number]
        move_x = jnp.dot(jnp.dot(row_modes, mixing[0]), col_modes.T)
        move_y = jnp.dot(jnp.dot(row_modes, mixing[1]), col_modes.T)
        pos_y = jnp.clip(row_coord + move_y, 0.0, HEIGHT - 1.0)
        pos_x = jnp.clip(col_coord + move_x, 0.0, COLUMNS - 1.0)
        floor_y = jnp.floor(pos_y)
        floor_x = jnp.floor(pos_x)
        frac_y = pos_y - floor_y
        frac_x = pos_x - floor_x
        low_y = floor_y.astype(jnp.int32)
        low_x = floor_x.astype(jnp.int32)
        high_y = jnp.minimum(low_y + 1, HEIGHT - 1)
        high_x = jnp.minimum(low_x + 1, COLUMNS - 1)
        sample = (1.0 - frac_y) * (1.0 - frac_x) * flat_texture[low_y * COLUMNS + low_x]
        sample = sample + (1.0 - frac_y) * frac_x * flat_texture[low_y * COLUMNS + high_x]
        sample = sample + frac_y * (1.0 - frac_x) * flat_texture[high_y * COLUMNS + low_x]
        sample = sample + frac_y * frac_x * flat_texture[high_y * COLUMNS + high_x]
        noise_field = jax.random.normal(jax.random.fold_in(key_list[3], slice_number), (HEIGHT, COLUMNS), jnp.float32)
        section_image = stains[slice_number] * gain_field * sample + background + noise_level * noise_field
        return jnp.clip(section_image, -8.0, 8.0)
    return lax.map(one_slice, jnp.arange(SLICES + 1, dtype=jnp.int32))


def draw_sections(key, part):
    return stack_helper(key)[1:].astype(jnp.bfloat16)


def draw_anchor(key, part):
    return stack_helper(key)[0].astype(jnp.bfloat16)


def setup_inputs(seed: int = 0) -> dict:
    streams_of = jax.random.split(jax.random.key(seed), 3)
    return {
        "sections": draw_sections(jax.random.fold_in(streams_of[2], 71), 0),
        "anchor": draw_anchor(jax.random.fold_in(streams_of[2], 71), 0),
    }


EPSILON = 1e-06
SMOOTHING = 0.25
EXACT_PRECISION = lax.Precision.HIGHEST

def spline_weight(offset):
    distance = jnp.abs(offset)
    near_part = 2.0 / 3.0 - distance * distance + 0.5 * distance * distance * distance
    remain = 2.0 - distance
    far_part = remain * remain * remain / 6.0
    return jnp.where(distance < 1.0, near_part, jnp.where(distance < 2.0, far_part, 0.0 * distance))

def spline_basis(first_row, pixel_count, extent):
    spacing = extent // GRID_SIZE
    pixels = (first_row + jnp.arange(pixel_count, dtype=jnp.int32)).astype(jnp.float32)
    knot_pos = jnp.arange(GRID_SIZE, dtype=jnp.int32).astype(jnp.float32)
    offset = (pixels[:, None] + 0.5) / spacing - knot_pos[None, :] - 0.5
    return spline_weight(offset)

def slopes(images):
    padded = jnp.pad(images, ((0, 0), (1, 1), (1, 1)))
    along_x = 0.5 * (padded[:, 1:-1, 2:] - padded[:, 1:-1, :-2])
    along_y = 0.5 * (padded[:, 2:, 1:-1] - padded[:, :-2, 1:-1])
    return (along_x, along_y)

def displace(coefficients, row_basis, col_half):
    row_mixed = jnp.einsum('hg,bgk->bhk', row_basis, coefficients, precision=EXACT_PRECISION)
    row_mixed = row_mixed.astype(jnp.bfloat16).astype(jnp.float32)
    col_wide = col_half.astype(jnp.float32)
    shift_x = jnp.einsum('bhg,wg->bhw', row_mixed[:, :, :GRID_SIZE], col_wide, precision=EXACT_PRECISION)
    shift_y = jnp.einsum('bhg,wg->bhw', row_mixed[:, :, GRID_SIZE:], col_wide, precision=EXACT_PRECISION)
    return (shift_x, shift_y)

def project(field_x, field_y, row_basis, col_half):
    col_wide = col_half.astype(jnp.float32)
    rounded_x = field_x.astype(jnp.bfloat16).astype(jnp.float32)
    rounded_y = field_y.astype(jnp.bfloat16).astype(jnp.float32)
    cols_x = jnp.einsum('bhw,wg->bhg', rounded_x, col_wide, precision=EXACT_PRECISION)
    cols_y = jnp.einsum('bhw,wg->bhg', rounded_y, col_wide, precision=EXACT_PRECISION)
    joined = jnp.concatenate([cols_x, cols_y], axis=2)
    return jnp.einsum('hg,bhk->bgk', row_basis, joined, precision=EXACT_PRECISION)

def normalized(gradient):
    magnitude = lax.optimization_barrier(jnp.mean(gradient * gradient, axis=(1, 2), keepdims=True))
    return gradient / jnp.sqrt(magnitude + EPSILON)

def ncc_direction(moving, fixed_image, coefficients, row_basis, col_half):
    along_x, along_y = slopes(moving)
    shift_x, shift_y = displace(coefficients, row_basis, col_half)
    warped = moving + shift_x * along_x + shift_y * along_y
    pixel_count = moving.shape[1] * moving.shape[2]
    centred_f = fixed_image - lax.optimization_barrier(jnp.mean(fixed_image, axis=(1, 2), keepdims=True))
    centred_m = warped - lax.optimization_barrier(jnp.mean(warped, axis=(1, 2), keepdims=True))
    moving_var = lax.optimization_barrier(jnp.sum(centred_m * centred_m, axis=(1, 2), keepdims=True))
    cross_var = lax.optimization_barrier(jnp.sum(centred_f * centred_m, axis=(1, 2), keepdims=True))
    denominator = jnp.sqrt(moving_var + EPSILON)
    ncc_score = cross_var / denominator
    pixel_grad = pixel_count * (centred_f / denominator - ncc_score / (moving_var + EPSILON) * centred_m)
    return normalized(project(pixel_grad * along_x, pixel_grad * along_y, row_basis, col_half))

def reference(sections, anchor):
    slice_total, height, columns = sections.shape
    row_basis = spline_basis(0, height, height)
    col_half = spline_basis(0, columns, columns).astype(jnp.bfloat16)
    step_rate = 1.0 / ITERATIONS
    previous = jnp.concatenate([anchor[None], sections[:-1]], axis=0)
    moving_blocks = sections.reshape(slice_total, 1, height, columns)
    fixed_blocks = previous.reshape(slice_total, 1, height, columns)
    coefficients = jnp.zeros((slice_total, GRID_SIZE, 2 * GRID_SIZE), jnp.float32)

    def one_block(packed):
        moving, fixed_image, block_coef = packed
        return ncc_direction(moving.astype(jnp.float32), fixed_image.astype(jnp.float32), block_coef, row_basis, col_half)
    for iteration in range(ITERATIONS):
        shaped = coefficients.reshape(slice_total, 1, GRID_SIZE, 2 * GRID_SIZE)
        direction = lax.map(one_block, (moving_blocks, fixed_blocks, shaped))
        direction = direction.reshape(slice_total, GRID_SIZE, 2 * GRID_SIZE)
        padded = jnp.pad(coefficients, ((1, 1), (0, 0), (0, 0)))
        smooth = padded[:-2] - 2.0 * coefficients + padded[2:]
        coefficients = coefficients + step_rate * direction + SMOOTHING * smooth
    accumulated = jnp.cumsum(coefficients, axis=0)

    def warp_block(packed):
        moving, block_coef = packed
        moving = moving.astype(jnp.float32)
        along_x, along_y = slopes(moving)
        shift_x, shift_y = displace(block_coef, row_basis, col_half)
        return (moving + shift_x * along_x + shift_y * along_y).astype(jnp.bfloat16)
    registered = lax.map(warp_block, (moving_blocks, accumulated.reshape(slice_total, 1, GRID_SIZE, 2 * GRID_SIZE)))
    registered = registered.reshape(slice_total, height, columns)
    return (registered, accumulated)
```

```python
import functools

import jax
import jax.numpy as jnp
from jax import lax
from jax.experimental import pallas as pl
from jax.experimental.pallas import tpu as pltpu
from jax.sharding import PartitionSpec as P

GRID_SIZE = 64
ITERATIONS = 4
EPSILON = 1e-06
SMOOTHING = 0.25
EXACT = lax.Precision.HIGHEST
BAND = 4
SPLIT = 4
LANES = 128
EDGE = 8
BLOCK_ROWS = 32
BLOCK_COLS = 512
VMEM_BYTES = 60 * 2**20


def spline_weight(offset):
    distance = jnp.abs(offset)
    near_part = 2.0 / 3.0 - distance * distance + 0.5 * distance * distance * distance
    remain = 2.0 - distance
    far_part = remain * remain * remain / 6.0
    return jnp.where(distance < 1.0, near_part, jnp.where(distance < 2.0, far_part, 0.0))


def spline_basis(first_row, pixel_count, extent):
    spacing = extent // GRID_SIZE
    pixels = (first_row + jnp.arange(pixel_count, dtype=jnp.int32)).astype(jnp.float32)
    knot_pos = jnp.arange(GRID_SIZE, dtype=jnp.int32).astype(jnp.float32)
    offset = (pixels[:, None] + 0.5) / spacing - knot_pos[None, :] - 0.5
    return spline_weight(offset)


def with_ends(array, axis, dim):
    size, length = lax.axis_size(axis), array.shape[dim]
    up = [(i, i + 1) for i in range(size - 1)]
    down = [(j, i) for i, j in up]
    before = lax.ppermute(lax.slice_in_dim(array, length - 1, length, axis=dim), axis, up)
    after = lax.ppermute(lax.slice_in_dim(array, 0, 1, axis=dim), axis, down)
    return before, after


def fill_wide(m_ref, edges_ref, wide):
    rows, cols = m_ref.shape
    height = rows + 2 * EDGE
    zeros = jnp.zeros((height, LANES), jnp.float32)
    wide[:, pl.ds(0, LANES)] = zeros
    wide[:, pl.ds(cols + LANES, LANES)] = zeros
    wide[pl.ds(0, EDGE), pl.ds(LANES, cols)] = edges_ref[pl.ds(0, EDGE), :]
    wide[pl.ds(EDGE + rows, EDGE), pl.ds(LANES, cols)] = edges_ref[pl.ds(EDGE, EDGE), :]

    @pl.loop(0, rows // BLOCK_ROWS)
    def _(i):
        r = pl.multiple_of(i * BLOCK_ROWS, BLOCK_ROWS)
        wide[pl.ds(EDGE + r, BLOCK_ROWS), pl.ds(LANES, cols)] = m_ref[
            pl.ds(r, BLOCK_ROWS), :
        ].astype(jnp.float32)


def slopes_of(wide, r, c):
    across = wide[pl.ds(r + EDGE, BLOCK_ROWS), pl.ds(c, BLOCK_COLS + 2 * LANES)]
    total = BLOCK_COLS + 2 * LANES
    slope_x = 0.5 * (pltpu.roll(across, total - 1, 1) - pltpu.roll(across, 1, 1))
    slope_x = slope_x[:, LANES : LANES + BLOCK_COLS]
    value = across[:, LANES : LANES + BLOCK_COLS]
    down = wide[pl.ds(r, BLOCK_ROWS + 2 * EDGE), pl.ds(c + LANES, BLOCK_COLS)]
    tall = BLOCK_ROWS + 2 * EDGE
    slope_y = 0.5 * (pltpu.roll(down, tall - 1, 0) - pltpu.roll(down, 1, 0))
    slope_y = slope_y[EDGE : EDGE + BLOCK_ROWS, :]
    return value, slope_x, slope_y


def fold(array):
    rows, cols = array.shape
    out = jnp.zeros((8, LANES), jnp.float32)
    for a in range(rows // 8):
        for b in range(cols // LANES):
            out = out + array[a * 8 : a * 8 + 8, b * LANES : b * LANES + LANES]
    return out


def warp_kernel(m_ref, edges_ref, mixed_ref, flat_ref, out_ref, wide, stage_x, stage_y):
    rows, cols = m_ref.shape
    fill_wide(m_ref, edges_ref, wide)
    span = stage_x.shape[1]

    @pl.loop(0, cols // span)
    def _(chunk):
        start = pl.multiple_of(chunk * span, span)
        flat = flat_ref[:, pl.ds(start, span)]
        stage_x[...] = jnp.dot(mixed_ref[:, :GRID_SIZE], flat, preferred_element_type=jnp.float32)
        stage_y[...] = jnp.dot(mixed_ref[:, GRID_SIZE:], flat, preferred_element_type=jnp.float32)
        per_row = span // BLOCK_COLS

        @pl.loop(0, rows // BLOCK_ROWS * per_row)
        def _(step):
            i, j = step // per_row, step % per_row
            r = pl.multiple_of(i * BLOCK_ROWS, BLOCK_ROWS)
            c = pl.multiple_of(j * BLOCK_COLS, BLOCK_COLS)
            value, sx, sy = slopes_of(wide, r, pl.multiple_of(start + c, BLOCK_COLS))
            here = (pl.ds(r, BLOCK_ROWS), pl.ds(c, BLOCK_COLS))
            out = value + stage_x[here] * sx + stage_y[here] * sy
            out_ref[pl.ds(r, BLOCK_ROWS), pl.ds(pl.multiple_of(start + c, BLOCK_COLS), BLOCK_COLS)] = (
                out.astype(jnp.bfloat16)
            )


def warp(moving, edges, mixed, flat):
    rows, cols = moving.shape
    vmem = pl.BlockSpec(memory_space=pltpu.VMEM)
    return pl.pallas_call(
        warp_kernel,
        out_shape=jax.ShapeDtypeStruct((rows, cols), jnp.bfloat16),
        in_specs=[vmem] * 4,
        out_specs=vmem,
        scratch_shapes=[
            pltpu.VMEM((rows + 2 * EDGE, cols + 2 * LANES), jnp.float32),
            pltpu.VMEM((rows, 1024), jnp.float32),
            pltpu.VMEM((rows, 1024), jnp.float32),
        ],
        compiler_params=pltpu.CompilerParams(vmem_limit_bytes=VMEM_BYTES),
    )(moving, edges, mixed, flat)


MESH = pl.DeviceIdType.MESH
HEAD = 8
HALO = 16
FIELDS = 7
SPAN = 1024
F32 = jnp.float32
BF16 = jnp.bfloat16


def window_of(knots):
    return 16 + max(8, -(-knots // 8) * 8)


def base_of(strip, knots):
    return lax.div(strip * knots, 8) * 8


def strip_basis(shape, pixel_dim, first_row, first_knot, spacing):
    pixels = (first_row + lax.broadcasted_iota(jnp.int32, shape, pixel_dim)).astype(F32)
    knot_pos = (first_knot + lax.broadcasted_iota(jnp.int32, shape, 1 - pixel_dim)).astype(F32)
    return spline_weight((pixels + 0.5) * (1.0 / spacing) - knot_pos - 0.5)


def column_tables(basis_ref, pairs_ref, spacing):
    middle = GRID_SIZE // 2
    wide = BAND * GRID_SIZE
    shape = (spacing, wide)
    lane = lax.broadcasted_iota(jnp.int32, shape, 1)
    pixel = (middle * spacing + lax.broadcasted_iota(jnp.int32, shape, 0)).astype(F32)
    place = (pixel + 0.5) * (1.0 / spacing) - 0.5
    knot, band = lax.rem(lane, GRID_SIZE), lax.div(lane, GRID_SIZE)
    rounded = lambda values: values.astype(BF16).astype(F32)
    single = rounded(spline_weight(place - knot.astype(F32)))
    product = single * rounded(spline_weight(place - (knot + band).astype(F32)))
    large = rounded(product)
    small = product - large
    one_lane = lax.broadcasted_iota(jnp.int32, (spacing, LANES), 1)
    one_knot = lax.rem(one_lane, GRID_SIZE)

    @pl.loop(0, GRID_SIZE)
    def _(t):
        at = pl.ds(pl.multiple_of(t * spacing, spacing), spacing)
        shift = lax.rem(t - middle + LANES, LANES)
        close = jnp.abs(one_knot - t) <= BAND
        moved = jnp.where(close, pltpu.roll(single[:, :LANES], shift, 1), 0.0)
        for k in range(2):
            half = one_lane < GRID_SIZE if k == 0 else one_lane >= GRID_SIZE
            basis_ref[k, at, :] = jnp.where(half, moved, 0.0).astype(BF16)
        for k in range(wide // LANES):
            cols = slice(k * LANES, (k + 1) * LANES)
            reach = one_knot + (k * LANES // GRID_SIZE + lax.div(one_lane, GRID_SIZE))
            keep = close & (reach < GRID_SIZE)
            for part, values in enumerate((large, small)):
                rolled = jnp.where(keep, pltpu.roll(values[:, cols], shift, 1), 0.0)
                pairs_ref[part, at, cols] = rolled.astype(BF16)


def fill_rows(wide, at, source, row, count, skip=0):
    cols = source.shape[1]
    values = source[pl.ds(row, count + skip), :].astype(F32)
    wide[pl.ds(at, count), pl.ds(LANES, cols)] = values[skip:]


def fill_body(wide, source, offset, rows):
    @pl.loop(0, rows // BLOCK_ROWS)
    def _(i):
        r = pl.multiple_of(i * BLOCK_ROWS, BLOCK_ROWS)
        fill_rows(wide, EDGE + r, source, pl.multiple_of(offset + r, 16), BLOCK_ROWS)


def blocks(rows, start, body):
    per_row = SPAN // BLOCK_COLS

    @pl.loop(0, rows // BLOCK_ROWS * per_row)
    def _(step):
        i, j = lax.div(step, per_row), lax.rem(step, per_row)
        r = pl.multiple_of(i * BLOCK_ROWS, BLOCK_ROWS)
        c = pl.multiple_of(j * BLOCK_COLS, BLOCK_COLS)
        body(r, c, pl.multiple_of(start + c, BLOCK_COLS))


def still_tables(wide, fields, basis_ref, pairs_ref, lin, raw, sums, rows, cols):
    dot = functools.partial(jnp.dot, preferred_element_type=F32)

    @pl.loop(0, cols // SPAN)
    def _(part):
        start = pl.multiple_of(part * SPAN, SPAN)

        def body(r, c, at):
            value, sx, sy = slopes_of(wide, r, at)
            here = (pl.ds(r, BLOCK_ROWS), pl.ds(c, BLOCK_COLS))
            for k, field in enumerate((value * sx, value * sy, sx, sy, sx * sx, sx * sy, sy * sy)):
                fields[(k, *here)] = field.astype(BF16)
            sums[1] += fold(value)
            sums[3] += fold(value * value)

        blocks(rows, start, body)
        cut = pl.ds(start, SPAN)
        for k in range(2):
            lin[1 + k] += dot(fields[2 * k], basis_ref[0, cut, :]) + dot(fields[2 * k + 1], basis_ref[1, cut, :])
        for k in range(3):
            raw[k] += dot(fields[4 + k], pairs_ref[0, cut, :]) + dot(fields[4 + k], pairs_ref[1, cut, :])


def rest_tables(wide, fixed, fixed_row, fields, basis_ref, lin, sums, rows, cols):
    dot = functools.partial(jnp.dot, preferred_element_type=F32)

    @pl.loop(0, cols // SPAN)
    def _(part):
        start = pl.multiple_of(part * SPAN, SPAN)

        def body(r, c, at):
            value, sx, sy = slopes_of(wide, r, at)
            f = fixed[pl.ds(pl.multiple_of(fixed_row + r, BLOCK_ROWS), BLOCK_ROWS), pl.ds(at, BLOCK_COLS)]
            f = f.astype(F32)
            rest = f - value
            here = (pl.ds(r, BLOCK_ROWS), pl.ds(c, BLOCK_COLS))
            fields[(0, *here)] = (rest * sx).astype(BF16)
            fields[(1, *here)] = (rest * sy).astype(BF16)
            sums[0] += fold(f)
            sums[2] += fold(rest * value)

        blocks(rows, start, body)
        cut = pl.ds(start, SPAN)
        here = pl.ds(0, rows)
        lin[0, here] += dot(fields[0, here], basis_ref[0, cut, :]) + dot(fields[1, here], basis_ref[1, cut, :])


def quad_tables(raw, quad):
    for d in range(BAND):
        at = slice(d * GRID_SIZE, (d + 1) * GRID_SIZE)
        xx, xy, yy = (raw[k, :, at] for k in range(3))
        quad[d] = jnp.concatenate([xx, yy], axis=1)
        quad[BAND + d] = jnp.concatenate([xy, xy], axis=1)


def head_rows(sums, keys):
    zero = jnp.zeros((1, LANES), F32)
    rows = [jnp.sum(sums[k], axis=0, keepdims=True) if k in keys else zero for k in range(4)]
    return jnp.concatenate(rows + [jnp.zeros((HEAD - 4, LANES), F32)], axis=0)


def grand(values):
    return jnp.sum(jnp.sum(values, axis=0, keepdims=True), axis=1, keepdims=True)


def track_kernel(strips, chain, m_ref, anchor_ref, acc_ref, mixed_ref, *scratch):
    (fixed, low, top, bottom, wide, fields, basis_ref, pairs_ref, lin, raw, quad, sums) = scratch[:12]
    (row_basis, row_basis_t, moved, hist, parts, side, near, ends, grads) = scratch[12:21]
    (quad_send, quad_recv, side_send, side_recv, near_send, near_recv) = scratch[21:27]
    (end_send, end_recv, bulk_send, bulk_recv, local_sem) = scratch[27:]
    rows, cols = m_ref.shape
    half = rows // 2
    me, link = lax.axis_index("quad"), lax.axis_index("chain")
    knots = GRID_SIZE // strips
    window = window_of(knots)
    spacing = rows * strips // GRID_SIZE
    pixel_count = float(rows * strips * cols)
    base = base_of(me, knots)
    first, last = link == 0, link == chain - 1
    steps = range(1, strips)

    def mesh_copy(src, dst, send, recv, to):
        return pltpu.make_async_remote_copy(
            src_ref=src, dst_ref=dst, send_sem=send, recv_sem=recv, device_id=to, device_id_type=MESH
        )

    barrier = pltpu.get_barrier_semaphore()

    def greet(to):
        pl.semaphore_signal(barrier, inc=1, device_id=to, device_id_type=MESH)

    for step in steps:
        greet({"quad": lax.rem(me + step, strips)})
    for step in range(1, chain):
        greet({"chain": lax.rem(link + step, chain)})
    for edge, to in ((last, link + 1), (first, link - 1)):

        @pl.when(jnp.logical_not(edge))
        def _():
            for step in steps:
                greet({"chain": to, "quad": lax.rem(me + step, strips)})

    load_anchor = pltpu.make_async_copy(anchor_ref, fixed, local_sem)

    @pl.when(first)
    def _():
        load_anchor.start()

    @pl.when(me == 0)
    def _():
        top[...] = jnp.zeros_like(top)

    @pl.when(me == strips - 1)
    def _():
        bottom[...] = jnp.zeros_like(bottom)
        low[pl.ds(HALO + half, HALO), :] = jnp.zeros((HALO, cols), BF16)

    @pl.when(first)
    def _():
        near[:, 0] = jnp.zeros_like(near[:, 0])
        side[...] = jnp.zeros_like(side)

    @pl.when(last)
    def _():
        near[:, 1] = jnp.zeros_like(near[:, 1])

    begin = me * rows
    row_basis[...] = strip_basis((rows, window), 0, begin, base - 8, spacing)
    row_basis_t[...] = strip_basis((window, rows), 1, begin, base - 8, spacing)
    for ref in (hist, grads, lin, raw, sums):
        ref[...] = jnp.zeros_like(ref)
    zeros = jnp.zeros((rows + 2 * EDGE, LANES), F32)
    wide[:, pl.ds(0, LANES)] = zeros
    wide[:, pl.ds(cols + LANES, LANES)] = zeros
    column_tables(basis_ref, pairs_ref, cols // GRID_SIZE)
    cross = jnp.where(first, 0, strips - 1) + jnp.where(last, 0, strips - 1)
    pl.semaphore_wait(barrier, strips - 1 + chain - 1 + cross)

    start_rows, end_rows = m_ref.at[pl.ds(0, HALO)], m_ref.at[pl.ds(rows - HALO, HALO)]
    to_top = mesh_copy(end_rows, top, bulk_send.at[0], bulk_recv.at[0], {"quad": me + 1})
    to_bottom = mesh_copy(start_rows, bottom, bulk_send.at[1], bulk_recv.at[1], {"quad": me - 1})
    up = mesh_copy(
        m_ref.at[pl.ds(0, half)], fixed.at[pl.ds(0, half)], bulk_send.at[2], bulk_recv.at[2], {"chain": link + 1}
    )
    down = mesh_copy(
        m_ref.at[pl.ds(half - HALO, half + HALO)],
        low.at[pl.ds(0, half + HALO)],
        bulk_send.at[3],
        bulk_recv.at[3],
        {"chain": link - 1},
    )
    across = mesh_copy(
        start_rows,
        low.at[pl.ds(HALO + half, HALO)],
        bulk_send.at[4],
        bulk_recv.at[4],
        {"chain": link - 1, "quad": me - 1},
    )
    inner_top, inner_bottom = me > 0, me < strips - 1
    later, earlier = jnp.logical_not(last), jnp.logical_not(first)
    pl.when(inner_bottom)(lambda: to_top.start())
    pl.when(inner_top)(lambda: to_bottom.start())
    pl.when(later)(lambda: up.start())
    pl.when(earlier)(lambda: down.start())
    pl.when(jnp.logical_and(earlier, inner_top))(lambda: across.start())

    fill_body(wide, m_ref, 0, rows)
    pl.when(inner_top)(lambda: to_top.wait_recv())
    pl.when(inner_bottom)(lambda: to_bottom.wait_recv())
    fill_rows(wide, 0, top, 0, EDGE, EDGE)
    wide[pl.ds(EDGE + rows, EDGE), pl.ds(LANES, cols)] = bottom[...].astype(F32)[:EDGE]

    still_tables(wide, fields, basis_ref, pairs_ref, lin, raw, sums, rows, cols)
    quad_tables(raw, quad)

    exact = functools.partial(jnp.dot, precision=EXACT, preferred_element_type=F32)

    @pl.when(first)
    def _():
        load_anchor.wait()
        rest_tables(wide, fixed, 0, fields, basis_ref, lin, sums, rows, cols)

    @pl.when(earlier)
    def _():
        up.wait_recv()
        rest_tables(wide, fixed, 0, fields, basis_ref, lin, sums, half, cols)

    parts[0, me, pl.ds(0, HEAD)] = head_rows(sums, (0, 1, 2, 3))
    for k in range(3):
        parts[0, me, pl.ds(HEAD + k * window, window)] = exact(row_basis_t[...], lin[k])

    def spread(turn, count):
        copies = []
        for step in steps:
            at = parts.at[turn, me, pl.ds(0, count)]
            to = {"quad": lax.rem(me + step, strips)}
            copies.append(mesh_copy(at, at, quad_send.at[turn, step], quad_recv.at[turn, me], to))
        for copy in copies:
            copy.start()
        return copies

    def gathered(turn, count):
        for step in steps:
            peer = lax.rem(me + step, strips)
            at = parts.at[turn, peer, pl.ds(0, count)]
            mesh_copy(at, at, quad_send.at[turn, step], quad_recv.at[turn, peer], {"quad": peer}).wait_recv()

    def side_copy(row, step):
        to = {"chain": link + 1, "quad": lax.rem(me + step, strips)}
        return mesh_copy(parts.at[ITERATIONS, me, pl.ds(0, HEAD + window)], side.at[row], side_send.at[step], side_recv.at[row], to)

    sends = spread(0, HEAD + 3 * window)

    @pl.when(later)
    def _():
        down.wait_recv()
        pl.when(inner_bottom)(lambda: across.wait_recv())
        fill_body(wide, low, HALO, half)
        fill_rows(wide, 0, low, 0, EDGE, EDGE)
        tail = low[pl.ds(HALO + half, HALO), :].astype(F32)
        wide[pl.ds(EDGE + half, EDGE), pl.ds(LANES, cols)] = tail[:EDGE]
        sums[...] = jnp.zeros_like(sums)
        lin[0] = jnp.zeros_like(lin[0])
        rest_tables(wide, m_ref, half, fields, basis_ref, lin, sums, half, cols)
        parts[ITERATIONS, me, pl.ds(0, HEAD)] = head_rows(sums, (0, 2))
        parts[ITERATIONS, me, pl.ds(HEAD, window)] = exact(row_basis_t[:, half:], lin[0, pl.ds(0, half)])
        for step in range(strips):
            side_copy(me, step).start()

    gathered(0, HEAD + 3 * window)

    @pl.when(earlier)
    def _():
        for step in range(strips):
            side_copy(lax.rem(me + step, strips), step).wait_recv()

    def near_copy(turn, side_of):
        to = {"chain": link + 1 if side_of == 0 else link - 1}
        src = hist.at[turn, pl.ds(8, GRID_SIZE)]
        return mesh_copy(src, near.at[turn, side_of], near_send.at[turn, side_of], near_recv.at[turn, side_of], to)

    def collect(ref, turn, offset, slot):
        for strip in range(strips):
            at = strip * knots // 8 * 8
            here = (strip, pl.ds(offset, window))
            grads[slot, pl.ds(at, window)] += ref[here] if turn is None else ref[(turn, *here)]
        return grads[slot, pl.ds(8, GRID_SIZE)]

    head = parts[0, 0, pl.ds(0, HEAD)] + side[0, pl.ds(0, HEAD)]
    for strip in steps:
        head = head + (parts[0, strip, pl.ds(0, HEAD)] + side[strip, pl.ds(0, HEAD)])
    head = jnp.sum(head, axis=1, keepdims=True)
    total = [head[k : k + 1, :] for k in range(4)]
    collect(side, None, HEAD, 0)
    grad_rest, grad_still, grad_ones = (collect(parts, 0, HEAD + k * window, k) for k in range(3))
    fixed_mean = total[0] / pixel_count
    block = 128

    for turn in range(ITERATIONS):
        moving_sum, moving_sq, cross_sum = total[1], total[3], total[2] + total[3]
        grad_extra = 0.0
        before = hist[turn, pl.ds(8, GRID_SIZE)]
        smooth = 0.0
        if turn:
            mixed_all = exact(row_basis[...], hist[turn, pl.ds(base, window)])
            moved[...] = mixed_all.astype(BF16).astype(F32)

            @pl.loop(0, rows // block)
            def _(i):
                r = pl.ds(pl.multiple_of(i * block, block), block)
                mixed = moved[r, :]
                other = pltpu.roll(mixed, GRID_SIZE, 1)
                out = quad[0, r, :] * mixed + quad[BAND, r, :] * other
                for d in range(1, BAND):
                    q, p = quad[d, r, :], quad[BAND + d, r, :]
                    out += q * pltpu.roll(mixed, LANES - d, 1) + p * pltpu.roll(other, LANES - d, 1)
                    out += pltpu.roll(q * mixed + p * other, d, 1)
                moved[r, :] = out

            parts[turn, me, pl.ds(0, window)] = exact(row_basis_t[...], moved[...])
            sends += spread(turn, window)
            gathered(turn, window)
            grad_extra = collect(parts, turn, 0, 2 + turn)
            moving_sum = moving_sum + grand(before * grad_ones)
            moving_sq = moving_sq + grand(before * (2.0 * grad_still + grad_extra))
            cross_sum = cross_sum + grand(before * (grad_rest + grad_still))
            pl.when(earlier)(lambda: near_copy(turn, 0).wait_recv())
            pl.when(later)(lambda: near_copy(turn, 1).wait_recv())
            smooth = near[turn, 0] - 2.0 * before + near[turn, 1]
        moving_mean = moving_sum / pixel_count
        moving_var = moving_sq - pixel_count * moving_mean * moving_mean
        cross_var = cross_sum - pixel_count * fixed_mean * moving_mean
        denominator = jnp.sqrt(moving_var + EPSILON)
        ratio = cross_var / denominator / (moving_var + EPSILON)
        gradient = pixel_count * (
            (grad_rest + grad_still - fixed_mean * grad_ones) / denominator
            - ratio * (grad_still + grad_extra - moving_mean * grad_ones)
        )
        size = grand(gradient * gradient) / (2.0 * GRID_SIZE * GRID_SIZE)
        direction = gradient / jnp.sqrt(size + EPSILON)
        hist[turn + 1, pl.ds(8, GRID_SIZE)] = before + direction / ITERATIONS + SMOOTHING * smooth
        if turn < ITERATIONS - 1:
            pl.when(later)(lambda: near_copy(turn + 1, 0).start())
            pl.when(earlier)(lambda: near_copy(turn + 1, 1).start())

    def end_copy(owner, step):
        src = hist.at[ITERATIONS, pl.ds(8, GRID_SIZE)]
        to = {"chain": lax.rem(link + step, chain)}
        return mesh_copy(src, ends.at[owner], end_send.at[step], end_recv.at[owner], to)

    for step in range(1, chain):
        end_copy(link, step).start()
    ends[link] = hist[ITERATIONS, pl.ds(8, GRID_SIZE)]
    for step in range(1, chain):
        end_copy(lax.rem(link + step, chain), step).wait_recv()
    out = ends[0]
    for owner in range(1, chain):
        out = out + jnp.where(owner <= link, ends[owner], 0.0)
    acc_ref[...] = out
    hist[0, pl.ds(8, GRID_SIZE)] = out
    mixed_ref[...] = exact(row_basis[...], hist[0, pl.ds(base, window)]).astype(BF16)
    for copy in sends:
        copy.wait_send()
    for turn in range(1, ITERATIONS):
        pl.when(later)(lambda: near_copy(turn, 0).wait_send())
        pl.when(earlier)(lambda: near_copy(turn, 1).wait_send())
    for step in range(1, chain):
        end_copy(link, step).wait_send()
    pl.when(inner_bottom)(lambda: to_top.wait_send())
    pl.when(inner_top)(lambda: to_bottom.wait_send())
    pl.when(earlier)(lambda: down.wait_send())
    pl.when(jnp.logical_and(earlier, inner_top))(lambda: across.wait_send())

    @pl.when(later)
    def _():
        up.wait_send()
        for step in range(strips):
            side_copy(me, step).wait_send()


def track(moving, anchor):
    rows, cols = moving.shape
    strips, chain = lax.axis_size("quad"), lax.axis_size("chain")
    window = window_of(GRID_SIZE // strips)
    vmem = pl.BlockSpec(memory_space=pltpu.VMEM)
    tall = GRID_SIZE + 16 + window
    dma = pltpu.SemaphoreType.DMA
    return pl.pallas_call(
        functools.partial(track_kernel, strips, chain),
        out_shape=(
            jax.ShapeDtypeStruct((GRID_SIZE, LANES), F32),
            jax.ShapeDtypeStruct((rows, LANES), BF16),
        ),
        in_specs=[vmem, pl.BlockSpec(memory_space=pl.ANY)],
        out_specs=[vmem] * 2,
        scratch_shapes=[
            pltpu.VMEM((rows, cols), BF16),
            pltpu.VMEM((rows // 2 + 2 * HALO, cols), BF16),
            pltpu.VMEM((HALO, cols), BF16),
            pltpu.VMEM((HALO, cols), BF16),
            pltpu.VMEM((rows + 2 * EDGE, cols + 2 * LANES), F32),
            pltpu.VMEM((FIELDS, rows, SPAN), BF16),
            pltpu.VMEM((2, cols, LANES), BF16),
            pltpu.VMEM((2, cols, BAND * GRID_SIZE), BF16),
            pltpu.VMEM((3, rows, LANES), F32),
            pltpu.VMEM((3, rows, BAND * GRID_SIZE), F32),
            pltpu.VMEM((2 * BAND, rows, LANES), F32),
            pltpu.VMEM((4, 8, LANES), F32),
            pltpu.VMEM((rows, window), F32),
            pltpu.VMEM((window, rows), F32),
            pltpu.VMEM((rows, LANES), F32),
            pltpu.VMEM((ITERATIONS + 1, tall, LANES), F32),
            pltpu.VMEM((ITERATIONS + 1, strips, HEAD + 3 * window, LANES), F32),
            pltpu.VMEM((strips, HEAD + window, LANES), F32),
            pltpu.VMEM((ITERATIONS + 1, 2, GRID_SIZE, LANES), F32),
            pltpu.VMEM((chain, GRID_SIZE, LANES), F32),
            pltpu.VMEM((ITERATIONS + 2, tall, LANES), F32),
            dma((ITERATIONS, strips)),
            dma((ITERATIONS, strips)),
            dma((strips,)),
            dma((strips,)),
            dma((ITERATIONS + 1, 2)),
            dma((ITERATIONS + 1, 2)),
            dma((chain,)),
            dma((chain,)),
            dma((5,)),
            dma((5,)),
            dma,
        ],
        compiler_params=pltpu.CompilerParams(
            collective_id=0, has_side_effects=True, vmem_limit_bytes=VMEM_BYTES
        ),
    )(moving, anchor)


def local(sections, anchor):
    _, rows, columns = sections.shape
    moving = sections[0]
    basis = spline_basis(0, columns, columns).astype(jnp.bfloat16)
    before, after = with_ends(moving, "quad", 0)
    edges = jnp.concatenate(
        [
            jnp.broadcast_to(before, (EDGE, columns)),
            jnp.broadcast_to(after, (EDGE, columns)),
        ],
        axis=0,
    ).astype(jnp.float32)
    accumulated, mixed = track(moving, anchor)
    registered = warp(moving, edges, mixed, basis.T)
    return registered[None], accumulated[None]


def solution(mesh):
    in_specs = (P("chain", "quad", None), P("quad", None))
    out_specs = (P("chain", "quad", None), P("chain", None, None))
    return jax.shard_map(local, mesh=mesh, in_specs=in_specs, out_specs=out_specs, check_vma=False)
```

```python
import functools

import jax
import jax.numpy as jnp
import numpy as np
from jax import lax
from jax.experimental import pallas as pl
from jax.experimental.pallas import tpu as pltpu
from jax.sharding import PartitionSpec as P

GRID_SIZE = 64
ITERATIONS = 4
EPSILON = 1e-06
SMOOTHING = 0.25
EXACT = lax.Precision.HIGHEST
BAND = 4
SPLIT = 4
LANES = 128
EDGE = 8
BLOCK_ROWS = 64
BLOCK_COLS = 1024
VMEM_BYTES = 60 * 2**20


def spline_weight(offset):
    distance = jnp.abs(offset)
    near_part = 2.0 / 3.0 - distance * distance + 0.5 * distance * distance * distance
    remain = 2.0 - distance
    far_part = remain * remain * remain / 6.0
    return jnp.where(distance < 1.0, near_part, jnp.where(distance < 2.0, far_part, 0.0))


def slopes_of(wide, r, c):
    across = wide[pl.ds(r + EDGE, BLOCK_ROWS), pl.ds(c, BLOCK_COLS + 2 * LANES)]
    total = BLOCK_COLS + 2 * LANES
    slope_x = pltpu.roll(across, total - 1, 1) - pltpu.roll(across, 1, 1)
    slope_x = slope_x[:, LANES : LANES + BLOCK_COLS]
    value = across[:, LANES : LANES + BLOCK_COLS]
    down = wide[pl.ds(r, BLOCK_ROWS + 2 * EDGE), pl.ds(c + LANES, BLOCK_COLS)]
    tall = BLOCK_ROWS + 2 * EDGE
    slope_y = pltpu.roll(down, tall - 1, 0) - pltpu.roll(down, 1, 0)
    slope_y = slope_y[EDGE : EDGE + BLOCK_ROWS, :]
    return value, slope_x, slope_y


def fold(array):
    rows, cols = array.shape
    out = jnp.zeros((8, LANES), jnp.float32)
    for a in range(rows // 8):
        for b in range(cols // LANES):
            out = out + array[a * 8 : a * 8 + 8, b * LANES : b * LANES + LANES]
    return out


def warp_kernel(above_ref, m_ref, below_ref, edges_ref, mixed_ref, flat_ref, out_ref, wide):
    step, rows, cols = pl.program_id(0), m_ref.shape[0], m_ref.shape[1]
    zeros = jnp.zeros((rows + 2 * EDGE, LANES), jnp.float32)
    wide[:, pl.ds(0, LANES)] = zeros
    wide[:, pl.ds(cols + LANES, LANES)] = zeros
    above = above_ref[...].astype(jnp.float32)[EDGE:]
    below = below_ref[...].astype(jnp.float32)[:EDGE]
    inner = pl.ds(LANES, cols)
    wide[pl.ds(0, EDGE), inner] = jnp.where(step == 0, edges_ref[pl.ds(0, EDGE), :], above)
    wide[pl.ds(EDGE + rows, EDGE), inner] = jnp.where(
        step == pl.num_programs(0) - 1, edges_ref[pl.ds(EDGE, EDGE), :], below
    )
    wide[pl.ds(EDGE, rows), inner] = m_ref[...].astype(jnp.float32)

    @pl.loop(0, cols // BLOCK_COLS)
    def _(j):
        c = pl.multiple_of(j * BLOCK_COLS, BLOCK_COLS)
        value, sx, sy = slopes_of(wide, 0, c)
        flat = flat_ref[:, pl.ds(c, BLOCK_COLS)]
        shift_x = jnp.dot(mixed_ref[:, :GRID_SIZE], flat, preferred_element_type=jnp.float32)
        shift_y = jnp.dot(mixed_ref[:, GRID_SIZE:], flat, preferred_element_type=jnp.float32)
        out_ref[:, pl.ds(c, BLOCK_COLS)] = (value + shift_x * sx + shift_y * sy).astype(jnp.bfloat16)


def warp(moving, edges, mixed, flat):
    rows, cols = moving.shape
    thin = 2 * EDGE
    ratio, last = BLOCK_ROWS // thin, rows // thin - 1
    whole = lambda shape: pl.BlockSpec(shape, lambda i: (0, 0))
    return pl.pallas_call(
        warp_kernel,
        grid=(rows // BLOCK_ROWS,),
        out_shape=jax.ShapeDtypeStruct((rows, cols), jnp.bfloat16),
        in_specs=[
            pl.BlockSpec((thin, cols), lambda i: (jnp.maximum(ratio * i - 1, 0), 0)),
            pl.BlockSpec((BLOCK_ROWS, cols), lambda i: (i, 0)),
            pl.BlockSpec((thin, cols), lambda i: (jnp.minimum(ratio * i + ratio, last), 0)),
            whole(edges.shape),
            pl.BlockSpec((BLOCK_ROWS, LANES), lambda i: (i, 0)),
            whole(flat.shape),
        ],
        out_specs=pl.BlockSpec((BLOCK_ROWS, cols), lambda i: (i, 0)),
        scratch_shapes=[pltpu.VMEM((BLOCK_ROWS + 2 * EDGE, cols + 2 * LANES), jnp.float32)],
        compiler_params=pltpu.CompilerParams(vmem_limit_bytes=VMEM_BYTES),
    )(moving, moving, moving, edges, mixed, flat)


MESH = pl.DeviceIdType.MESH
HEAD = 8
HALO = 16
FIELDS = 7
SPAN = 1024
F32 = jnp.float32
BF16 = jnp.bfloat16


def window_of(knots):
    return 16 + max(8, -(-knots // 8) * 8)


def base_of(strip, knots):
    return lax.div(strip * knots, 8) * 8


def flat_table(cols):
    pixels = np.arange(cols, dtype=np.float32)[None, :]
    knots = np.arange(GRID_SIZE, dtype=np.float32)[:, None]
    offset = (pixels + np.float32(0.5)) / np.float32(cols // GRID_SIZE) - knots - np.float32(0.5)
    distance = np.abs(offset)
    near = np.float32(2.0 / 3.0) - distance * distance + np.float32(0.5) * distance * distance * distance
    remain = np.float32(2.0) - distance
    far = remain * remain * remain / np.float32(6.0)
    return np.where(distance < 1, near, np.where(distance < 2, far, np.float32(0))).astype(BF16)


def strip_basis(shape, pixel_dim, first_row, first_knot, spacing):
    pixels = (first_row + lax.broadcasted_iota(jnp.int32, shape, pixel_dim)).astype(F32)
    knot_pos = (first_knot + lax.broadcasted_iota(jnp.int32, shape, 1 - pixel_dim)).astype(F32)
    return spline_weight((pixels + 0.5) * (1.0 / spacing) - knot_pos - 0.5)


def column_tables(basis_ref, pairs_ref, spacing):
    middle = GRID_SIZE // 2
    wide = BAND * GRID_SIZE
    shape = (spacing, wide)
    lane = lax.broadcasted_iota(jnp.int32, shape, 1)
    pixel = (middle * spacing + lax.broadcasted_iota(jnp.int32, shape, 0)).astype(F32)
    place = (pixel + 0.5) * (1.0 / spacing) - 0.5
    knot, band = lax.rem(lane, GRID_SIZE), lax.div(lane, GRID_SIZE)
    rounded = lambda values: values.astype(BF16).astype(F32)
    single = rounded(spline_weight(place - knot.astype(F32)))
    product = single * rounded(spline_weight(place - (knot + band).astype(F32)))
    large = rounded(product)
    small = product - large
    one_lane = lax.broadcasted_iota(jnp.int32, (spacing, LANES), 1)
    one_knot = lax.rem(one_lane, GRID_SIZE)

    @pl.loop(0, GRID_SIZE)
    def _(t):
        at = pl.ds(pl.multiple_of(t * spacing, spacing), spacing)
        shift = lax.rem(t - middle + LANES, LANES)
        close = jnp.abs(one_knot - t) <= BAND
        moved = jnp.where(close, pltpu.roll(single[:, :LANES], shift, 1), 0.0)
        for k in range(2):
            half = one_lane < GRID_SIZE if k == 0 else one_lane >= GRID_SIZE
            basis_ref[k, at, :] = jnp.where(half, moved, 0.0).astype(BF16)
        for k in range(wide // LANES):
            cols = slice(k * LANES, (k + 1) * LANES)
            reach = one_knot + (k * LANES // GRID_SIZE + lax.div(one_lane, GRID_SIZE))
            keep = close & (reach < GRID_SIZE)
            for part, values in enumerate((large, small)):
                rolled = jnp.where(keep, pltpu.roll(values[:, cols], shift, 1), 0.0)
                pairs_ref[part, at, cols] = rolled.astype(BF16)


def fill_rows(wide, at, source, row, count, skip=0):
    cols = source.shape[1]
    values = source[pl.ds(row, count + skip), :].astype(F32)
    wide[pl.ds(at, count), pl.ds(LANES, cols)] = values[skip:]


def fill_body(wide, source, offset, rows):
    @pl.loop(0, rows // BLOCK_ROWS)
    def _(i):
        r = pl.multiple_of(i * BLOCK_ROWS, BLOCK_ROWS)
        fill_rows(wide, EDGE + r, source, pl.multiple_of(offset + r, 16), BLOCK_ROWS)


def blocks(rows, start, body):
    per_row = SPAN // BLOCK_COLS

    @pl.loop(0, rows // BLOCK_ROWS * per_row)
    def _(step):
        i, j = lax.div(step, per_row), lax.rem(step, per_row)
        r = pl.multiple_of(i * BLOCK_ROWS, BLOCK_ROWS)
        c = pl.multiple_of(j * BLOCK_COLS, BLOCK_COLS)
        body(r, c, pl.multiple_of(start + c, BLOCK_COLS))


def still_tables(wide, fields, basis_ref, pairs_ref, lin, raw, sums, rows, cols):
    dot = functools.partial(jnp.dot, preferred_element_type=F32)

    @pl.loop(0, cols // SPAN)
    def _(part):
        start = pl.multiple_of(part * SPAN, SPAN)

        def body(r, c, at):
            value, sx, sy = slopes_of(wide, r, at)
            here = (pl.ds(r, BLOCK_ROWS), pl.ds(c, BLOCK_COLS))
            for k, field in enumerate((value * sx, value * sy, sx, sy, sx * sx, sx * sy, sy * sy)):
                fields[(k, *here)] = field.astype(BF16)
            sums[1] += fold(value)
            sums[3] += fold(value * value)

        blocks(rows, start, body)
        cut = pl.ds(start, SPAN)
        for k in range(2):
            lin[1 + k] += dot(fields[2 * k], basis_ref[0, cut, :]) + dot(fields[2 * k + 1], basis_ref[1, cut, :])
        for k in range(3):
            raw[k] += dot(fields[4 + k], pairs_ref[0, cut, :]) + dot(fields[4 + k], pairs_ref[1, cut, :])


def rest_tables(wide, fixed, fixed_row, fields, basis_ref, lin, sums, rows, cols):
    dot = functools.partial(jnp.dot, preferred_element_type=F32)

    @pl.loop(0, cols // SPAN)
    def _(part):
        start = pl.multiple_of(part * SPAN, SPAN)

        def body(r, c, at):
            value, sx, sy = slopes_of(wide, r, at)
            f = fixed[pl.ds(pl.multiple_of(fixed_row + r, BLOCK_ROWS), BLOCK_ROWS), pl.ds(at, BLOCK_COLS)]
            f = f.astype(F32)
            rest = f - value
            here = (pl.ds(r, BLOCK_ROWS), pl.ds(c, BLOCK_COLS))
            fields[(0, *here)] = (rest * sx).astype(BF16)
            fields[(1, *here)] = (rest * sy).astype(BF16)
            sums[0] += fold(f)
            sums[2] += fold(rest * value)

        blocks(rows, start, body)
        cut = pl.ds(start, SPAN)
        here = pl.ds(0, rows)
        lin[0, here] += dot(fields[0, here], basis_ref[0, cut, :]) + dot(fields[1, here], basis_ref[1, cut, :])


def quad_tables(raw, quad):
    for d in range(BAND):
        at = slice(d * GRID_SIZE, (d + 1) * GRID_SIZE)
        xx, xy, yy = (0.25 * raw[k, :, at] for k in range(3))
        quad[d] = jnp.concatenate([xx, yy], axis=1)
        quad[BAND + d] = jnp.concatenate([xy, xy], axis=1)


def head_rows(sums, keys):
    zero = jnp.zeros((1, LANES), F32)
    rows = [jnp.sum(sums[k], axis=0, keepdims=True) if k in keys else zero for k in range(4)]
    return jnp.concatenate(rows + [jnp.zeros((HEAD - 4, LANES), F32)], axis=0)


def grand(values):
    return jnp.sum(jnp.sum(values, axis=0, keepdims=True), axis=1, keepdims=True)


def track_kernel(strips, chain, m_ref, anchor_ref, acc_ref, mixed_ref, edges_ref, *scratch):
    (fixed, low, top, bottom, wide, fields, basis_ref, pairs_ref, lin, raw, quad, sums) = scratch[:12]
    (row_basis, row_basis_t, moved, hist, parts, side, near, ends, grads) = scratch[12:21]
    (quad_send, quad_recv, side_send, side_recv, near_send, near_recv) = scratch[21:27]
    (end_send, end_recv, bulk_send, bulk_recv, local_sem) = scratch[27:]
    rows, cols = m_ref.shape
    half = rows // 2
    me, link = lax.axis_index("quad"), lax.axis_index("chain")
    knots = GRID_SIZE // strips
    window = window_of(knots)
    spacing = rows * strips // GRID_SIZE
    pixel_count = float(rows * strips * cols)
    base = base_of(me, knots)
    first, last = link == 0, link == chain - 1
    steps = range(1, strips)

    def mesh_copy(src, dst, send, recv, to):
        return pltpu.make_async_remote_copy(
            src_ref=src, dst_ref=dst, send_sem=send, recv_sem=recv, device_id=to, device_id_type=MESH
        )

    barrier = pltpu.get_barrier_semaphore()

    def greet(to):
        pl.semaphore_signal(barrier, inc=1, device_id=to, device_id_type=MESH)

    for step in steps:
        greet({"quad": lax.rem(me + step, strips)})
    for step in range(1, chain):
        greet({"chain": lax.rem(link + step, chain)})
    for edge, to in ((last, link + 1), (first, link - 1)):

        @pl.when(jnp.logical_not(edge))
        def _():
            for step in steps:
                greet({"chain": to, "quad": lax.rem(me + step, strips)})

    load_anchor = pltpu.make_async_copy(anchor_ref, fixed, local_sem)

    @pl.when(first)
    def _():
        load_anchor.start()

    @pl.when(me == 0)
    def _():
        top[...] = jnp.zeros_like(top)

    @pl.when(me == strips - 1)
    def _():
        bottom[...] = jnp.zeros_like(bottom)
        low[pl.ds(HALO + half, HALO), :] = jnp.zeros((HALO, cols), BF16)

    @pl.when(first)
    def _():
        near[:, 0] = jnp.zeros_like(near[:, 0])
        side[...] = jnp.zeros_like(side)

    @pl.when(last)
    def _():
        near[:, 1] = jnp.zeros_like(near[:, 1])

    begin = me * rows
    row_basis[...] = strip_basis((rows, window), 0, begin, base - 8, spacing)
    row_basis_t[...] = strip_basis((window, rows), 1, begin, base - 8, spacing)
    for ref in (hist, grads, lin, raw, sums):
        ref[...] = jnp.zeros_like(ref)
    zeros = jnp.zeros((rows + 2 * EDGE, LANES), F32)
    wide[:, pl.ds(0, LANES)] = zeros
    wide[:, pl.ds(cols + LANES, LANES)] = zeros
    column_tables(basis_ref, pairs_ref, cols // GRID_SIZE)
    cross = jnp.where(first, 0, strips - 1) + jnp.where(last, 0, strips - 1)
    pl.semaphore_wait(barrier, strips - 1 + chain - 1 + cross)

    start_rows, end_rows = m_ref.at[pl.ds(0, HALO)], m_ref.at[pl.ds(rows - HALO, HALO)]
    to_top = mesh_copy(end_rows, top, bulk_send.at[0], bulk_recv.at[0], {"quad": me + 1})
    to_bottom = mesh_copy(start_rows, bottom, bulk_send.at[1], bulk_recv.at[1], {"quad": me - 1})
    up = mesh_copy(
        m_ref.at[pl.ds(0, half)], fixed.at[pl.ds(0, half)], bulk_send.at[2], bulk_recv.at[2], {"chain": link + 1}
    )
    down = mesh_copy(
        m_ref.at[pl.ds(half - HALO, half + HALO)],
        low.at[pl.ds(0, half + HALO)],
        bulk_send.at[3],
        bulk_recv.at[3],
        {"chain": link - 1},
    )
    across = mesh_copy(
        start_rows,
        low.at[pl.ds(HALO + half, HALO)],
        bulk_send.at[4],
        bulk_recv.at[4],
        {"chain": link - 1, "quad": me - 1},
    )
    inner_top, inner_bottom = me > 0, me < strips - 1
    later, earlier = jnp.logical_not(last), jnp.logical_not(first)
    pl.when(inner_bottom)(lambda: to_top.start())
    pl.when(inner_top)(lambda: to_bottom.start())
    pl.when(later)(lambda: up.start())
    pl.when(earlier)(lambda: down.start())
    pl.when(jnp.logical_and(earlier, inner_top))(lambda: across.start())

    fill_body(wide, m_ref, 0, rows)
    pl.when(inner_top)(lambda: to_top.wait_recv())
    pl.when(inner_bottom)(lambda: to_bottom.wait_recv())
    for k, values in enumerate((top[...].astype(F32)[EDGE:], bottom[...].astype(F32)[:EDGE])):
        edges_ref[pl.ds(k * EDGE, EDGE), :] = values
        wide[pl.ds(k * (EDGE + rows), EDGE), pl.ds(LANES, cols)] = values

    still_tables(wide, fields, basis_ref, pairs_ref, lin, raw, sums, rows, cols)
    quad_tables(raw, quad)

    exact = functools.partial(jnp.dot, precision=EXACT, preferred_element_type=F32)

    @pl.when(first)
    def _():
        load_anchor.wait()
        rest_tables(wide, fixed, 0, fields, basis_ref, lin, sums, rows, cols)

    @pl.when(earlier)
    def _():
        up.wait_recv()
        rest_tables(wide, fixed, 0, fields, basis_ref, lin, sums, half, cols)

    parts[0, me, pl.ds(0, HEAD)] = head_rows(sums, (0, 1, 2, 3))
    for k in range(3):
        parts[0, me, pl.ds(HEAD + k * window, window)] = 0.5 * exact(row_basis_t[...], lin[k])

    def spread(turn, count):
        copies = []
        for step in steps:
            at = parts.at[turn, me, pl.ds(0, count)]
            to = {"quad": lax.rem(me + step, strips)}
            copies.append(mesh_copy(at, at, quad_send.at[turn, step], quad_recv.at[turn, me], to))
        for copy in copies:
            copy.start()
        return copies

    def gathered(turn, count):
        for step in steps:
            peer = lax.rem(me + step, strips)
            at = parts.at[turn, peer, pl.ds(0, count)]
            mesh_copy(at, at, quad_send.at[turn, step], quad_recv.at[turn, peer], {"quad": peer}).wait_recv()

    def side_copy(row, step):
        to = {"chain": link + 1, "quad": lax.rem(me + step, strips)}
        return mesh_copy(parts.at[ITERATIONS, me, pl.ds(0, HEAD + window)], side.at[row], side_send.at[step], side_recv.at[row], to)

    sends = spread(0, HEAD + 3 * window)

    @pl.when(later)
    def _():
        down.wait_recv()
        pl.when(inner_bottom)(lambda: across.wait_recv())
        fill_body(wide, low, HALO, half)
        fill_rows(wide, 0, low, 0, EDGE, EDGE)
        tail = low[pl.ds(HALO + half, HALO), :].astype(F32)
        wide[pl.ds(EDGE + half, EDGE), pl.ds(LANES, cols)] = tail[:EDGE]
        sums[...] = jnp.zeros_like(sums)
        lin[0] = jnp.zeros_like(lin[0])
        rest_tables(wide, m_ref, half, fields, basis_ref, lin, sums, half, cols)
        parts[ITERATIONS, me, pl.ds(0, HEAD)] = head_rows(sums, (0, 2))
        parts[ITERATIONS, me, pl.ds(HEAD, window)] = 0.5 * exact(row_basis_t[:, half:], lin[0, pl.ds(0, half)])
        for step in range(strips):
            side_copy(me, step).start()

    gathered(0, HEAD + 3 * window)

    @pl.when(earlier)
    def _():
        for step in range(strips):
            side_copy(lax.rem(me + step, strips), step).wait_recv()

    def near_copy(turn, side_of):
        to = {"chain": link + 1 if side_of == 0 else link - 1}
        src = hist.at[turn, pl.ds(8, GRID_SIZE)]
        return mesh_copy(src, near.at[turn, side_of], near_send.at[turn, side_of], near_recv.at[turn, side_of], to)

    def collect(ref, turn, offset, slot):
        for strip in range(strips):
            at = strip * knots // 8 * 8
            here = (strip, pl.ds(offset, window))
            grads[slot, pl.ds(at, window)] += ref[here] if turn is None else ref[(turn, *here)]
        return grads[slot, pl.ds(8, GRID_SIZE)]

    head = parts[0, 0, pl.ds(0, HEAD)] + side[0, pl.ds(0, HEAD)]
    for strip in steps:
        head = head + (parts[0, strip, pl.ds(0, HEAD)] + side[strip, pl.ds(0, HEAD)])
    head = jnp.sum(head, axis=1, keepdims=True)
    total = [head[k : k + 1, :] for k in range(4)]
    collect(side, None, HEAD, 0)
    grad_rest, grad_still, grad_ones = (collect(parts, 0, HEAD + k * window, k) for k in range(3))
    fixed_mean = total[0] / pixel_count
    block = 128

    for turn in range(ITERATIONS):
        moving_sum, moving_sq, cross_sum = total[1], total[3], total[2] + total[3]
        grad_extra = 0.0
        before = hist[turn, pl.ds(8, GRID_SIZE)]
        smooth = 0.0
        if turn:
            mixed_all = exact(row_basis[...], hist[turn, pl.ds(base, window)])
            moved[...] = mixed_all.astype(BF16).astype(F32)

            @pl.loop(0, rows // block)
            def _(i):
                r = pl.ds(pl.multiple_of(i * block, block), block)
                mixed = moved[r, :]
                other = pltpu.roll(mixed, GRID_SIZE, 1)
                out = quad[0, r, :] * mixed + quad[BAND, r, :] * other
                for d in range(1, BAND):
                    q, p = quad[d, r, :], quad[BAND + d, r, :]
                    out += q * pltpu.roll(mixed, LANES - d, 1) + p * pltpu.roll(other, LANES - d, 1)
                    out += pltpu.roll(q * mixed + p * other, d, 1)
                moved[r, :] = out

            parts[turn, me, pl.ds(0, window)] = exact(row_basis_t[...], moved[...])
            sends += spread(turn, window)
            gathered(turn, window)
            grad_extra = collect(parts, turn, 0, 2 + turn)
            moving_sum = moving_sum + grand(before * grad_ones)
            moving_sq = moving_sq + grand(before * (2.0 * grad_still + grad_extra))
            cross_sum = cross_sum + grand(before * (grad_rest + grad_still))
            pl.when(earlier)(lambda: near_copy(turn, 0).wait_recv())
            pl.when(later)(lambda: near_copy(turn, 1).wait_recv())
            smooth = near[turn, 0] - 2.0 * before + near[turn, 1]
        moving_mean = moving_sum / pixel_count
        moving_var = moving_sq - pixel_count * moving_mean * moving_mean
        cross_var = cross_sum - pixel_count * fixed_mean * moving_mean
        denominator = jnp.sqrt(moving_var + EPSILON)
        ratio = cross_var / denominator / (moving_var + EPSILON)
        gradient = pixel_count * (
            (grad_rest + grad_still - fixed_mean * grad_ones) / denominator
            - ratio * (grad_still + grad_extra - moving_mean * grad_ones)
        )
        size = grand(gradient * gradient) / (2.0 * GRID_SIZE * GRID_SIZE)
        direction = gradient / jnp.sqrt(size + EPSILON)
        hist[turn + 1, pl.ds(8, GRID_SIZE)] = before + direction / ITERATIONS + SMOOTHING * smooth
        if turn < ITERATIONS - 1:
            pl.when(later)(lambda: near_copy(turn + 1, 0).start())
            pl.when(earlier)(lambda: near_copy(turn + 1, 1).start())

    def end_copy(owner, step):
        src = hist.at[ITERATIONS, pl.ds(8, GRID_SIZE)]
        to = {"chain": lax.rem(link + step, chain)}
        return mesh_copy(src, ends.at[owner], end_send.at[step], end_recv.at[owner], to)

    for step in range(1, chain):
        end_copy(link, step).start()
    ends[link] = hist[ITERATIONS, pl.ds(8, GRID_SIZE)]
    for step in range(1, chain):
        end_copy(lax.rem(link + step, chain), step).wait_recv()
    out = ends[0]
    for owner in range(1, chain):
        out = out + jnp.where(owner <= link, ends[owner], 0.0)
    acc_ref[...] = out
    hist[0, pl.ds(8, GRID_SIZE)] = out
    mixed_ref[...] = exact(row_basis[...], hist[0, pl.ds(base, window)]).astype(BF16) * jnp.asarray(0.5, BF16)
    for copy in sends:
        copy.wait_send()
    for turn in range(1, ITERATIONS):
        pl.when(later)(lambda: near_copy(turn, 0).wait_send())
        pl.when(earlier)(lambda: near_copy(turn, 1).wait_send())
    for step in range(1, chain):
        end_copy(link, step).wait_send()
    pl.when(inner_bottom)(lambda: to_top.wait_send())
    pl.when(inner_top)(lambda: to_bottom.wait_send())
    pl.when(earlier)(lambda: down.wait_send())
    pl.when(jnp.logical_and(earlier, inner_top))(lambda: across.wait_send())

    @pl.when(later)
    def _():
        up.wait_send()
        for step in range(strips):
            side_copy(me, step).wait_send()


def track(moving, anchor):
    rows, cols = moving.shape
    strips, chain = lax.axis_size("quad"), lax.axis_size("chain")
    window = window_of(GRID_SIZE // strips)
    vmem = pl.BlockSpec(memory_space=pltpu.VMEM)
    tall = GRID_SIZE + 16 + window
    dma = pltpu.SemaphoreType.DMA
    return pl.pallas_call(
        functools.partial(track_kernel, strips, chain),
        out_shape=(
            jax.ShapeDtypeStruct((GRID_SIZE, LANES), F32),
            jax.ShapeDtypeStruct((rows, LANES), BF16),
            jax.ShapeDtypeStruct((2 * EDGE, cols), F32),
        ),
        in_specs=[vmem, pl.BlockSpec(memory_space=pl.ANY)],
        out_specs=[vmem] * 3,
        scratch_shapes=[
            pltpu.VMEM((rows, cols), BF16),
            pltpu.VMEM((rows // 2 + 2 * HALO, cols), BF16),
            pltpu.VMEM((HALO, cols), BF16),
            pltpu.VMEM((HALO, cols), BF16),
            pltpu.VMEM((rows + 2 * EDGE, cols + 2 * LANES), F32),
            pltpu.VMEM((FIELDS, rows, SPAN), BF16),
            pltpu.VMEM((2, cols, LANES), BF16),
            pltpu.VMEM((2, cols, BAND * GRID_SIZE), BF16),
            pltpu.VMEM((3, rows, LANES), F32),
            pltpu.VMEM((3, rows, BAND * GRID_SIZE), F32),
            pltpu.VMEM((2 * BAND, rows, LANES), F32),
            pltpu.VMEM((4, 8, LANES), F32),
            pltpu.VMEM((rows, window), F32),
            pltpu.VMEM((window, rows), F32),
            pltpu.VMEM((rows, LANES), F32),
            pltpu.VMEM((ITERATIONS + 1, tall, LANES), F32),
            pltpu.VMEM((ITERATIONS + 1, strips, HEAD + 3 * window, LANES), F32),
            pltpu.VMEM((strips, HEAD + window, LANES), F32),
            pltpu.VMEM((ITERATIONS + 1, 2, GRID_SIZE, LANES), F32),
            pltpu.VMEM((chain, GRID_SIZE, LANES), F32),
            pltpu.VMEM((ITERATIONS + 2, tall, LANES), F32),
            dma((ITERATIONS, strips)),
            dma((ITERATIONS, strips)),
            dma((strips,)),
            dma((strips,)),
            dma((ITERATIONS + 1, 2)),
            dma((ITERATIONS + 1, 2)),
            dma((chain,)),
            dma((chain,)),
            dma((5,)),
            dma((5,)),
            dma,
        ],
        compiler_params=pltpu.CompilerParams(
            collective_id=0, has_side_effects=True, vmem_limit_bytes=VMEM_BYTES
        ),
    )(moving, anchor)


def local(sections, anchor):
    moving = sections[0]
    accumulated, mixed, edges = track(moving, anchor)
    registered = warp(moving, edges, mixed, flat_table(moving.shape[1]))
    return registered[None], accumulated[None]


def solution(mesh):
    in_specs = (P("chain", "quad", None), P("quad", None))
    out_specs = (P("chain", "quad", None), P("chain", None, None))
    return jax.shard_map(local, mesh=mesh, in_specs=in_specs, out_specs=out_specs, check_vma=False)
```

```python
import functools

import jax
import jax.numpy as jnp
import numpy as np
from jax import lax
from jax.experimental import pallas as pl
from jax.experimental.pallas import tpu as pltpu
from jax.sharding import PartitionSpec as P

GRID_SIZE = 64
ITERATIONS = 4
EPSILON = 1e-06
SMOOTHING = 0.25
BAND = 4
SPLIT = 4
LANES = 128
EDGE = 8
BLOCK_ROWS = 64
BLOCK_COLS = 1024
VMEM_BYTES = 60 * 2**20


def spline_weight(offset):
    distance = jnp.abs(offset)
    near_part = 2.0 / 3.0 - distance * distance + 0.5 * distance * distance * distance
    remain = 2.0 - distance
    far_part = remain * remain * remain / 6.0
    return jnp.where(distance < 1.0, near_part, jnp.where(distance < 2.0, far_part, 0.0))


def slopes_of(wide, r, c):
    across = wide[pl.ds(r + EDGE, BLOCK_ROWS), pl.ds(c, BLOCK_COLS + 2 * LANES)]
    total = BLOCK_COLS + 2 * LANES
    slope_x = pltpu.roll(across, total - 1, 1) - pltpu.roll(across, 1, 1)
    slope_x = slope_x[:, LANES : LANES + BLOCK_COLS]
    value = across[:, LANES : LANES + BLOCK_COLS]
    down = wide[pl.ds(r, BLOCK_ROWS + 2 * EDGE), pl.ds(c + LANES, BLOCK_COLS)]
    tall = BLOCK_ROWS + 2 * EDGE
    slope_y = pltpu.roll(down, tall - 1, 0) - pltpu.roll(down, 1, 0)
    slope_y = slope_y[EDGE : EDGE + BLOCK_ROWS, :]
    return value, slope_x, slope_y


def fold(array):
    rows, cols = array.shape
    out = jnp.zeros((8, LANES), jnp.float32)
    for a in range(rows // 8):
        for b in range(cols // LANES):
            out = out + array[a * 8 : a * 8 + 8, b * LANES : b * LANES + LANES]
    return out


def warp_kernel(above_ref, m_ref, below_ref, edges_ref, mixed_ref, flat_ref, out_ref, wide):
    step, rows, cols = pl.program_id(0), m_ref.shape[0], m_ref.shape[1]
    zeros = jnp.zeros((rows + 2 * EDGE, LANES), jnp.float32)
    wide[:, pl.ds(0, LANES)] = zeros
    wide[:, pl.ds(cols + LANES, LANES)] = zeros
    above = above_ref[...].astype(jnp.float32)[EDGE:]
    below = below_ref[...].astype(jnp.float32)[:EDGE]
    inner = pl.ds(LANES, cols)
    wide[pl.ds(0, EDGE), inner] = jnp.where(step == 0, edges_ref[pl.ds(0, EDGE), :], above)
    wide[pl.ds(EDGE + rows, EDGE), inner] = jnp.where(
        step == pl.num_programs(0) - 1, edges_ref[pl.ds(EDGE, EDGE), :], below
    )
    wide[pl.ds(EDGE, rows), inner] = m_ref[...].astype(jnp.float32)

    @pl.loop(0, cols // BLOCK_COLS)
    def _(j):
        c = pl.multiple_of(j * BLOCK_COLS, BLOCK_COLS)
        value, sx, sy = slopes_of(wide, 0, c)
        flat = flat_ref[:, pl.ds(c, BLOCK_COLS)]
        shift_x = jnp.dot(mixed_ref[:, :GRID_SIZE], flat, preferred_element_type=jnp.float32)
        shift_y = jnp.dot(mixed_ref[:, GRID_SIZE:], flat, preferred_element_type=jnp.float32)
        out_ref[:, pl.ds(c, BLOCK_COLS)] = (value + shift_x * sx + shift_y * sy).astype(jnp.bfloat16)


def warp(moving, edges, mixed, flat):
    rows, cols = moving.shape
    thin = 2 * EDGE
    ratio, last = BLOCK_ROWS // thin, rows // thin - 1
    whole = lambda shape: pl.BlockSpec(shape, lambda i: (0, 0))
    return pl.pallas_call(
        warp_kernel,
        grid=(rows // BLOCK_ROWS,),
        out_shape=jax.ShapeDtypeStruct((rows, cols), jnp.bfloat16),
        in_specs=[
            pl.BlockSpec((thin, cols), lambda i: (jnp.maximum(ratio * i - 1, 0), 0)),
            pl.BlockSpec((BLOCK_ROWS, cols), lambda i: (i, 0)),
            pl.BlockSpec((thin, cols), lambda i: (jnp.minimum(ratio * i + ratio, last), 0)),
            whole(edges.shape),
            pl.BlockSpec((BLOCK_ROWS, LANES), lambda i: (i, 0)),
            whole(flat.shape),
        ],
        out_specs=pl.BlockSpec((BLOCK_ROWS, cols), lambda i: (i, 0)),
        scratch_shapes=[pltpu.VMEM((BLOCK_ROWS + 2 * EDGE, cols + 2 * LANES), jnp.float32)],
        compiler_params=pltpu.CompilerParams(vmem_limit_bytes=VMEM_BYTES),
    )(moving, moving, moving, edges, mixed, flat)


MESH = pl.DeviceIdType.MESH
HEAD = 8
HALO = 16
FIELDS = 7
SPAN = 1024
F32 = jnp.float32
BF16 = jnp.bfloat16


def window_of(knots):
    return 16 + max(8, -(-knots // 8) * 8)


def narrow_of(knots):
    return -(-(knots + 8) // 8) * 8


def base_of(strip, knots):
    return lax.div(strip * knots, 8) * 8


def flat_table(cols):
    pixels = np.arange(cols, dtype=np.float32)[None, :]
    knots = np.arange(GRID_SIZE, dtype=np.float32)[:, None]
    offset = (pixels + np.float32(0.5)) / np.float32(cols // GRID_SIZE) - knots - np.float32(0.5)
    distance = np.abs(offset)
    near = np.float32(2.0 / 3.0) - distance * distance + np.float32(0.5) * distance * distance * distance
    remain = np.float32(2.0) - distance
    far = remain * remain * remain / np.float32(6.0)
    return np.where(distance < 1, near, np.where(distance < 2, far, np.float32(0))).astype(BF16)


def strip_basis(shape, pixel_dim, first_row, first_knot, spacing):
    pixels = (first_row + lax.broadcasted_iota(jnp.int32, shape, pixel_dim)).astype(F32)
    knot_pos = (first_knot + lax.broadcasted_iota(jnp.int32, shape, 1 - pixel_dim)).astype(F32)
    return spline_weight((pixels + 0.5) * (1.0 / spacing) - knot_pos - 0.5)


def column_tables(basis_ref, pairs_ref, spacing):
    middle = GRID_SIZE // 2
    wide = BAND * GRID_SIZE
    shape = (spacing, wide)
    lane = lax.broadcasted_iota(jnp.int32, shape, 1)
    pixel = (middle * spacing + lax.broadcasted_iota(jnp.int32, shape, 0)).astype(F32)
    place = (pixel + 0.5) * (1.0 / spacing) - 0.5
    knot, band = lax.rem(lane, GRID_SIZE), lax.div(lane, GRID_SIZE)
    rounded = lambda values: values.astype(BF16).astype(F32)
    single = rounded(spline_weight(place - knot.astype(F32)))
    product = single * rounded(spline_weight(place - (knot + band).astype(F32)))
    one_lane = lax.broadcasted_iota(jnp.int32, (spacing, LANES), 1)
    one_knot = lax.rem(one_lane, GRID_SIZE)

    @pl.loop(0, GRID_SIZE)
    def _(t):
        at = pl.ds(pl.multiple_of(t * spacing, spacing), spacing)
        shift = lax.rem(t - middle + LANES, LANES)
        close = jnp.abs(one_knot - t) <= BAND
        moved = jnp.where(close, pltpu.roll(single[:, :LANES], shift, 1), 0.0)
        for k in range(2):
            half = one_lane < GRID_SIZE if k == 0 else one_lane >= GRID_SIZE
            basis_ref[k, at, :] = jnp.where(half, moved, 0.0).astype(BF16)
        for k in range(wide // LANES):
            cols = slice(k * LANES, (k + 1) * LANES)
            reach = one_knot + (k * LANES // GRID_SIZE + lax.div(one_lane, GRID_SIZE))
            keep = close & (reach < GRID_SIZE)
            rolled = jnp.where(keep, pltpu.roll(product[:, cols], shift, 1), 0.0)
            pairs_ref[at, cols] = rolled.astype(BF16)


def fill_rows(wide, at, source, row, count, skip=0):
    cols = source.shape[1]
    values = source[pl.ds(row, count + skip), :].astype(F32)
    wide[pl.ds(at, count), pl.ds(LANES, cols)] = values[skip:]


def fill_body(wide, source, offset, rows):
    @pl.loop(0, rows // BLOCK_ROWS)
    def _(i):
        r = pl.multiple_of(i * BLOCK_ROWS, BLOCK_ROWS)
        fill_rows(wide, EDGE + r, source, pl.multiple_of(offset + r, 16), BLOCK_ROWS)


def blocks(rows, start, body):
    per_row = SPAN // BLOCK_COLS

    @pl.loop(0, rows // BLOCK_ROWS * per_row)
    def _(step):
        i, j = lax.div(step, per_row), lax.rem(step, per_row)
        r = pl.multiple_of(i * BLOCK_ROWS, BLOCK_ROWS)
        c = pl.multiple_of(j * BLOCK_COLS, BLOCK_COLS)
        body(r, c, pl.multiple_of(start + c, BLOCK_COLS))


def still_tables(wide, fields, basis_ref, pairs_ref, lin, raw, sums, rows, cols):
    dot = functools.partial(jnp.dot, preferred_element_type=F32)

    @pl.loop(0, cols // SPAN)
    def _(part):
        start = pl.multiple_of(part * SPAN, SPAN)

        def body(r, c, at):
            value, sx, sy = slopes_of(wide, r, at)
            here = (pl.ds(r, BLOCK_ROWS), pl.ds(c, BLOCK_COLS))
            for k, field in enumerate((value * sx, value * sy, sx, sy, sx * sx, sx * sy, sy * sy)):
                fields[(k, *here)] = field.astype(BF16)
            sums[1] += fold(value)
            sums[3] += fold(value * value)

        blocks(rows, start, body)
        cut = pl.ds(start, SPAN)
        for k in range(2):
            lin[1 + k] += dot(fields[2 * k], basis_ref[0, cut, :]) + dot(fields[2 * k + 1], basis_ref[1, cut, :])
        for k in range(3):
            raw[k] += dot(fields[4 + k], pairs_ref[cut, :])


def rest_tables(wide, fixed, fixed_row, fields, basis_ref, lin, sums, rows, cols, target=0):
    dot = functools.partial(jnp.dot, preferred_element_type=F32)

    @pl.loop(0, cols // SPAN)
    def _(part):
        start = pl.multiple_of(part * SPAN, SPAN)

        def body(r, c, at):
            value, sx, sy = slopes_of(wide, r, at)
            f = fixed[pl.ds(pl.multiple_of(fixed_row + r, BLOCK_ROWS), BLOCK_ROWS), pl.ds(at, BLOCK_COLS)]
            f = f.astype(F32)
            rest = f - value
            here = (pl.ds(r, BLOCK_ROWS), pl.ds(c, BLOCK_COLS))
            fields[(0, *here)] = (rest * sx).astype(BF16)
            fields[(1, *here)] = (rest * sy).astype(BF16)
            sums[0] += fold(f)
            sums[2] += fold(rest * value)

        blocks(rows, start, body)
        cut = pl.ds(start, SPAN)
        here = pl.ds(0, rows)
        lin[0, pl.ds(target, rows)] += dot(fields[0, here], basis_ref[0, cut, :]) + dot(
            fields[1, here], basis_ref[1, cut, :]
        )


def quad_tables(raw, quad):
    for d in range(BAND):
        at = slice(d * GRID_SIZE, (d + 1) * GRID_SIZE)
        xx, xy, yy = (0.25 * raw[k, :, at] for k in range(3))
        quad[d] = jnp.concatenate([xx, yy], axis=1)
        quad[BAND + d] = jnp.concatenate([xy, xy], axis=1)


def head_rows(sums, keys):
    zero = jnp.zeros((1, LANES), F32)
    rows = [jnp.sum(sums[k], axis=0, keepdims=True) if k in keys else zero for k in range(4)]
    return jnp.concatenate(rows + [jnp.zeros((HEAD - 4, LANES), F32)], axis=0)


def thirds(values):
    high = values.astype(BF16).astype(F32)
    rest = values - high
    middle = rest.astype(BF16).astype(F32)
    return high, middle, (rest - middle).astype(BF16).astype(F32)


def mix(row_six, control):
    high, middle, low = thirds(control)
    six = jnp.concatenate([high, middle, high, low, middle, high], axis=0).astype(BF16)
    return jnp.dot(row_six[...], six, preferred_element_type=F32)


def project_rows(row_three, values):
    window = row_three.shape[0] // 3
    out = 0.0
    for k, part in enumerate(thirds(values)):
        product = jnp.dot(row_three[...], part.astype(BF16), preferred_element_type=F32)
        for j in range(3 - k):
            out += product[j * window : (j + 1) * window]
    return out


def grand(values):
    return jnp.sum(jnp.sum(values, axis=0, keepdims=True), axis=1, keepdims=True)


def track_kernel(strips, chain, m_ref, anchor_ref, acc_ref, mixed_ref, edges_ref, *scratch):
    (fixed, low, top, bottom, tail, first_row, last_row, wide, low_wide, fields, basis_ref, pairs_ref, lin, raw, quad, sums) = scratch[:16]
    (row_six, row_three, moved, hist, parts, side, near, ends, grads) = scratch[16:25]
    (quad_send, quad_recv, side_send, side_recv, near_send, near_recv) = scratch[25:31]
    (end_send, end_recv, bulk_send, bulk_recv, local_sem) = scratch[31:]
    rows, cols = m_ref.shape
    half = rows // 2
    me, link = lax.axis_index("quad"), lax.axis_index("chain")
    knots = GRID_SIZE // strips
    window, narrow = window_of(knots), narrow_of(knots)
    early = ITERATIONS + 1
    spacing = rows * strips // GRID_SIZE
    pixel_count = float(rows * strips * cols)
    base = base_of(me, knots)
    first, last = link == 0, link == chain - 1
    steps = range(1, strips)

    def mesh_copy(src, dst, send, recv, to):
        return pltpu.make_async_remote_copy(
            src_ref=src, dst_ref=dst, send_sem=send, recv_sem=recv, device_id=to, device_id_type=MESH
        )

    barrier = pltpu.get_barrier_semaphore()

    def greet(to):
        pl.semaphore_signal(barrier, inc=1, device_id=to, device_id_type=MESH)

    for step in steps:
        greet({"quad": lax.rem(me + step, strips)})
    for step in range(1, chain):
        greet({"chain": lax.rem(link + step, chain)})
    for edge, to in ((last, link + 1), (first, link - 1)):

        @pl.when(jnp.logical_not(edge))
        def _():
            for step in steps:
                greet({"chain": to, "quad": lax.rem(me + step, strips)})

    load_anchor = pltpu.make_async_copy(anchor_ref, fixed, local_sem)

    @pl.when(first)
    def _():
        load_anchor.start()

    first_row[...] = m_ref[pl.ds(0, HALO), :].astype(F32)[:1]
    last_row[...] = m_ref[pl.ds(rows - HALO, HALO), :].astype(F32)[HALO - 1 :]
    begin = me * rows
    lane = lax.broadcasted_iota(jnp.int32, (rows, 6 * window), 1)
    group = sum((lane >= k * window).astype(jnp.int32) for k in range(1, 6))
    pixels = (begin + lax.broadcasted_iota(jnp.int32, (rows, 6 * window), 0)).astype(F32)
    knot_pos = (base - 8 + lane - window * group).astype(F32)
    high, middle, small = thirds(spline_weight((pixels + 0.5) * (1.0 / spacing) - knot_pos - 0.5))
    is_middle = (group == 2) | (group == 4)
    row_six[...] = jnp.where(group == 5, small, jnp.where(is_middle, middle, high)).astype(BF16)
    rows_t = thirds(strip_basis((narrow, rows), 1, begin, me * knots - 4, spacing))
    row_three[...] = jnp.concatenate(rows_t, axis=0).astype(BF16)
    fill_body(wide, m_ref, 0, rows)
    cross = jnp.where(first, 0, strips - 1) + jnp.where(last, 0, strips - 1)
    pl.semaphore_wait(barrier, strips - 1 + chain - 1 + cross)

    to_top = mesh_copy(last_row, top, bulk_send.at[0], bulk_recv.at[0], {"quad": me + 1})
    to_bottom = mesh_copy(first_row, bottom, bulk_send.at[1], bulk_recv.at[1], {"quad": me - 1})
    def up(count):
        at = pl.ds(0, count)
        return mesh_copy(m_ref.at[at], fixed.at[at], bulk_send.at[2], bulk_recv.at[2], {"chain": link + 1})

    def down(count):
        source = m_ref.at[pl.ds(rows - count - HALO, count + HALO)]
        target = low.at[pl.ds(half - count, count + HALO)]
        return mesh_copy(source, target, bulk_send.at[3], bulk_recv.at[3], {"chain": link - 1})

    across = mesh_copy(
        first_row,
        tail,
        bulk_send.at[4],
        bulk_recv.at[4],
        {"chain": link - 1, "quad": me - 1},
    )
    inner_top, inner_bottom = me > 0, me < strips - 1
    later, earlier = jnp.logical_not(last), jnp.logical_not(first)
    even = lax.rem(link, 2) == 0
    odd = jnp.logical_not(even)
    wide_share = 3 * rows // 4
    pl.when(inner_bottom)(lambda: to_top.start())
    pl.when(inner_top)(lambda: to_bottom.start())
    pl.when(later & even)(lambda: up(wide_share).start())
    pl.when(later & odd)(lambda: up(half).start())
    pl.when(earlier & odd)(lambda: down(rows - wide_share).start())
    pl.when(earlier & even)(lambda: down(half).start())
    pl.when(jnp.logical_and(earlier, inner_top))(lambda: across.start())

    @pl.when(me == 0)
    def _():
        top[...] = jnp.zeros_like(top)

    @pl.when(me == strips - 1)
    def _():
        bottom[...] = jnp.zeros_like(bottom)
        tail[...] = jnp.zeros_like(tail)

    @pl.when(first)
    def _():
        near[:, 0] = jnp.zeros_like(near[:, 0])
        side[...] = jnp.zeros_like(side)

    @pl.when(last)
    def _():
        near[:, 1] = jnp.zeros_like(near[:, 1])

    for ref in (hist, grads, lin, raw, sums):
        ref[...] = jnp.zeros_like(ref)
    zeros = jnp.zeros((rows + 2 * EDGE, LANES), F32)
    for at in (0, cols + LANES):
        wide[:, pl.ds(at, LANES)] = zeros
        low_wide[:, pl.ds(at, LANES)] = zeros[: half + 2 * EDGE]
    column_tables(basis_ref, pairs_ref, cols // GRID_SIZE)
    pl.when(inner_top)(lambda: to_top.wait_recv())
    pl.when(inner_bottom)(lambda: to_bottom.wait_recv())
    for k, row in enumerate((top, bottom)):
        values = jnp.broadcast_to(row[...], (EDGE, cols))
        edges_ref[pl.ds(k * EDGE, EDGE), :] = values
        wide[pl.ds(k * (EDGE + rows), EDGE), pl.ds(LANES, cols)] = values

    still_tables(wide, fields, basis_ref, pairs_ref, lin, raw, sums, rows, cols)
    quad_tables(raw, quad)

    def spread(turn, count):
        copies = []
        for step in steps:
            at = parts.at[turn, me, pl.ds(0, count)]
            to = {"quad": lax.rem(me + step, strips)}
            copies.append(mesh_copy(at, at, quad_send.at[turn, step], quad_recv.at[turn, me], to))
        for copy in copies:
            copy.start()
        return copies

    def gathered(turn, count):
        for step in steps:
            peer = lax.rem(me + step, strips)
            at = parts.at[turn, peer, pl.ds(0, count)]
            mesh_copy(at, at, quad_send.at[turn, step], quad_recv.at[turn, peer], {"quad": peer}).wait_recv()

    def side_copy(row, step):
        to = {"chain": link + 1, "quad": lax.rem(me + step, strips)}
        return mesh_copy(parts.at[ITERATIONS, me, pl.ds(0, HEAD + narrow)], side.at[row], side_send.at[step], side_recv.at[row], to)

    still_sums = (1, 3)

    def own_part(wait, count):
        wait()
        sums[...] = jnp.zeros_like(sums)
        rest_tables(wide, fixed, 0, fields, basis_ref, lin, sums, count, cols)
        parts[0, me, pl.ds(HEAD, narrow)] = 0.5 * project_rows(row_three, lin[0])
        parts[0, me, pl.ds(0, HEAD)] = head_rows(sums, (0, 2))

    def later_part(count):
        down(count).wait_recv()
        pl.when(inner_bottom)(lambda: across.wait_recv())
        fill_body(low_wide, low, HALO + half - count, count)
        begin_low = half - count
        fill_rows(low_wide, 0, low, begin_low, EDGE, EDGE)
        low_wide[pl.ds(EDGE + count, EDGE), pl.ds(LANES, cols)] = jnp.broadcast_to(tail[...], (EDGE, cols))
        sums[...] = jnp.zeros_like(sums)
        lin[1] = jnp.zeros_like(lin[1])
        rest_tables(low_wide, m_ref, rows - count, fields, basis_ref, lin.at[pl.ds(1, 1)], sums, count, cols, rows - count)
        parts[ITERATIONS, me, pl.ds(0, HEAD)] = head_rows(sums, (0, 2))
        parts[ITERATIONS, me, pl.ds(HEAD, narrow)] = 0.5 * project_rows(row_three, lin[1])
        for step in range(strips):
            side_copy(me, step).start()

    parts[early, me, pl.ds(0, HEAD)] = head_rows(sums, still_sums)
    for k in range(2):
        parts[early, me, pl.ds(HEAD + k * narrow, narrow)] = 0.5 * project_rows(row_three, lin[1 + k])
    sends = spread(early, HEAD + 2 * narrow)
    pl.when(even & later)(lambda: later_part(rows - wide_share))
    pl.when(first)(lambda: own_part(load_anchor.wait, rows))
    pl.when(even & earlier)(lambda: own_part(up(half).wait_recv, half))
    pl.when(odd)(lambda: own_part(up(wide_share).wait_recv, wide_share))
    sends += spread(0, HEAD + narrow)
    pl.when(odd & later)(lambda: later_part(half))
    gathered(early, HEAD + 2 * narrow)
    gathered(0, HEAD + narrow)

    @pl.when(earlier)
    def _():
        for step in range(strips):
            side_copy(lax.rem(me + step, strips), step).wait_recv()

    def near_copy(turn, side_of):
        to = {"chain": link + 1 if side_of == 0 else link - 1}
        src = hist.at[turn, pl.ds(8, GRID_SIZE)]
        return mesh_copy(src, near.at[turn, side_of], near_send.at[turn, side_of], near_recv.at[turn, side_of], to)

    def collect(ref, turn, offset, slot):
        for strip in range(strips):
            here = (strip, pl.ds(offset, narrow))
            grads[slot, pl.ds(strip * knots + 4, narrow)] += ref[here] if turn is None else ref[(turn, *here)]
        return grads[slot, pl.ds(8, GRID_SIZE)]

    at = pl.ds(0, HEAD)
    head = 0.0
    for strip in range(strips):
        head = head + (parts[0, strip, at] + parts[early, strip, at] + side[strip, at])
    head = jnp.sum(head, axis=1, keepdims=True)
    total = [head[k : k + 1, :] for k in range(4)]
    collect(side, None, HEAD, 0)
    grad_rest = collect(parts, 0, HEAD, 0)
    grad_still, grad_ones = (collect(parts, early, HEAD + k * narrow, 1 + k) for k in range(2))
    fixed_mean = total[0] / pixel_count
    block = 128

    for turn in range(ITERATIONS):
        moving_sum, moving_sq, cross_sum = total[1], total[3], total[2] + total[3]
        grad_extra = 0.0
        before = hist[turn, pl.ds(8, GRID_SIZE)]
        smooth = 0.0
        if turn:
            mixed_all = mix(row_six, hist[turn, pl.ds(base, window)])
            moved[...] = mixed_all.astype(BF16).astype(F32)

            @pl.loop(0, rows // block)
            def _(i):
                r = pl.ds(pl.multiple_of(i * block, block), block)
                mixed = moved[r, :]
                other = pltpu.roll(mixed, GRID_SIZE, 1)
                out = quad[0, r, :] * mixed + quad[BAND, r, :] * other
                for d in range(1, BAND):
                    q, p = quad[d, r, :], quad[BAND + d, r, :]
                    out += q * pltpu.roll(mixed, LANES - d, 1) + p * pltpu.roll(other, LANES - d, 1)
                    out += pltpu.roll(q * mixed + p * other, d, 1)
                moved[r, :] = out

            parts[turn, me, pl.ds(0, narrow)] = project_rows(row_three, moved[...])
            sends += spread(turn, narrow)
            gathered(turn, narrow)
            grad_extra = collect(parts, turn, 0, 2 + turn)
            moving_sum = moving_sum + grand(before * grad_ones)
            moving_sq = moving_sq + grand(before * (2.0 * grad_still + grad_extra))
            cross_sum = cross_sum + grand(before * (grad_rest + grad_still))
            pl.when(earlier)(lambda: near_copy(turn, 0).wait_recv())
            pl.when(later)(lambda: near_copy(turn, 1).wait_recv())
            smooth = near[turn, 0] - 2.0 * before + near[turn, 1]
        moving_mean = moving_sum / pixel_count
        moving_var = moving_sq - pixel_count * moving_mean * moving_mean
        cross_var = cross_sum - pixel_count * fixed_mean * moving_mean
        denominator = jnp.sqrt(moving_var + EPSILON)
        ratio = cross_var / denominator / (moving_var + EPSILON)
        gradient = pixel_count * (
            (grad_rest + grad_still - fixed_mean * grad_ones) / denominator
            - ratio * (grad_still + grad_extra - moving_mean * grad_ones)
        )
        size = grand(gradient * gradient) / (2.0 * GRID_SIZE * GRID_SIZE)
        direction = gradient / jnp.sqrt(size + EPSILON)
        hist[turn + 1, pl.ds(8, GRID_SIZE)] = before + direction / ITERATIONS + SMOOTHING * smooth
        if turn < ITERATIONS - 1:
            pl.when(later)(lambda: near_copy(turn + 1, 0).start())
            pl.when(earlier)(lambda: near_copy(turn + 1, 1).start())

    def end_copy(owner, step):
        src = hist.at[ITERATIONS, pl.ds(8, GRID_SIZE)]
        to = {"chain": lax.rem(link + step, chain)}
        return mesh_copy(src, ends.at[owner], end_send.at[step], end_recv.at[owner], to)

    for step in range(1, chain):
        end_copy(link, step).start()
    ends[link] = hist[ITERATIONS, pl.ds(8, GRID_SIZE)]
    for step in range(1, chain):
        end_copy(lax.rem(link + step, chain), step).wait_recv()
    out = ends[0]
    for owner in range(1, chain):
        out = out + jnp.where(owner <= link, ends[owner], 0.0)
    acc_ref[...] = out
    hist[0, pl.ds(8, GRID_SIZE)] = out
    mixed_ref[...] = mix(row_six, hist[0, pl.ds(base, window)]).astype(BF16) * jnp.asarray(0.5, BF16)
    for copy in sends:
        copy.wait_send()
    for turn in range(1, ITERATIONS):
        pl.when(later)(lambda: near_copy(turn, 0).wait_send())
        pl.when(earlier)(lambda: near_copy(turn, 1).wait_send())
    for step in range(1, chain):
        end_copy(link, step).wait_send()
    pl.when(inner_bottom)(lambda: to_top.wait_send())
    pl.when(inner_top)(lambda: to_bottom.wait_send())
    pl.when(earlier & odd)(lambda: down(rows - wide_share).wait_send())
    pl.when(earlier & even)(lambda: down(half).wait_send())
    pl.when(later & even)(lambda: up(wide_share).wait_send())
    pl.when(later & odd)(lambda: up(half).wait_send())
    pl.when(jnp.logical_and(earlier, inner_top))(lambda: across.wait_send())

    @pl.when(later)
    def _():
        for step in range(strips):
            side_copy(me, step).wait_send()


def track(moving, anchor):
    rows, cols = moving.shape
    strips, chain = lax.axis_size("quad"), lax.axis_size("chain")
    window = window_of(GRID_SIZE // strips)
    vmem = pl.BlockSpec(memory_space=pltpu.VMEM)
    tall = GRID_SIZE + 16 + window
    dma = pltpu.SemaphoreType.DMA
    return pl.pallas_call(
        functools.partial(track_kernel, strips, chain),
        out_shape=(
            jax.ShapeDtypeStruct((GRID_SIZE, LANES), F32),
            jax.ShapeDtypeStruct((rows, LANES), BF16),
            jax.ShapeDtypeStruct((2 * EDGE, cols), F32),
        ),
        in_specs=[vmem, pl.BlockSpec(memory_space=pl.ANY)],
        out_specs=[vmem] * 3,
        scratch_shapes=[
            pltpu.VMEM((rows, cols), BF16),
            pltpu.VMEM((rows // 2 + HALO, cols), BF16),
        ]
        + [pltpu.VMEM((1, cols), F32)] * 5
        + [
            pltpu.VMEM((rows + 2 * EDGE, cols + 2 * LANES), F32),
            pltpu.VMEM((rows // 2 + 2 * EDGE, cols + 2 * LANES), F32),
            pltpu.VMEM((FIELDS, rows, SPAN), BF16),
            pltpu.VMEM((2, cols, LANES), BF16),
            pltpu.VMEM((cols, BAND * GRID_SIZE), BF16),
            pltpu.VMEM((3, rows, LANES), F32),
            pltpu.VMEM((3, rows, BAND * GRID_SIZE), F32),
            pltpu.VMEM((2 * BAND, rows, LANES), F32),
            pltpu.VMEM((4, 8, LANES), F32),
            pltpu.VMEM((rows, 6 * window), BF16),
            pltpu.VMEM((3 * narrow_of(GRID_SIZE // strips), rows), BF16),
            pltpu.VMEM((rows, LANES), F32),
            pltpu.VMEM((ITERATIONS + 1, tall, LANES), F32),
            pltpu.VMEM((ITERATIONS + 2, strips, HEAD + 2 * narrow_of(GRID_SIZE // strips), LANES), F32),
            pltpu.VMEM((strips, HEAD + narrow_of(GRID_SIZE // strips), LANES), F32),
            pltpu.VMEM((ITERATIONS + 1, 2, GRID_SIZE, LANES), F32),
            pltpu.VMEM((chain, GRID_SIZE, LANES), F32),
            pltpu.VMEM((ITERATIONS + 2, tall, LANES), F32),
            dma((ITERATIONS + 2, strips)),
            dma((ITERATIONS + 2, strips)),
            dma((strips,)),
            dma((strips,)),
            dma((ITERATIONS + 1, 2)),
            dma((ITERATIONS + 1, 2)),
            dma((chain,)),
            dma((chain,)),
            dma((5,)),
            dma((5,)),
            dma,
        ],
        compiler_params=pltpu.CompilerParams(
            collective_id=0, has_side_effects=True, vmem_limit_bytes=VMEM_BYTES
        ),
    )(moving, anchor)


def local(sections, anchor):
    moving = sections[0]
    accumulated, mixed, edges = track(moving, anchor)
    registered = warp(moving, edges, mixed, flat_table(moving.shape[1]))
    return registered[None], accumulated[None]


def solution(mesh):
    in_specs = (P("chain", "quad", None), P("quad", None))
    out_specs = (P("chain", "quad", None), P("chain", None, None))
    return jax.shard_map(local, mesh=mesh, in_specs=in_specs, out_specs=out_specs, check_vma=False)
```

```python
import functools

import jax
import jax.numpy as jnp
import numpy as np
from jax import lax
from jax.experimental import pallas as pl
from jax.experimental.pallas import tpu as pltpu
from jax.sharding import PartitionSpec as P

GRID_SIZE = 64
ITERATIONS = 4
EPSILON = 1e-06
SMOOTHING = 0.25
BAND = 4
SPLIT = 4
LANES = 128
EDGE = 8
BLOCK_ROWS = 64
BLOCK_COLS = 1024
VMEM_BYTES = 60 * 2**20


def spline_weight(offset):
    distance = jnp.abs(offset)
    near_part = 2.0 / 3.0 - distance * distance + 0.5 * distance * distance * distance
    remain = 2.0 - distance
    far_part = remain * remain * remain / 6.0
    return jnp.where(distance < 1.0, near_part, jnp.where(distance < 2.0, far_part, 0.0))


def slopes_of(wide, r, c):
    across = wide[pl.ds(r + EDGE, BLOCK_ROWS), pl.ds(c, BLOCK_COLS + 2 * LANES)]
    total = BLOCK_COLS + 2 * LANES
    slope_x = pltpu.roll(across, total - 1, 1) - pltpu.roll(across, 1, 1)
    slope_x = slope_x[:, LANES : LANES + BLOCK_COLS]
    value = across[:, LANES : LANES + BLOCK_COLS]
    down = wide[pl.ds(r, BLOCK_ROWS + 2 * EDGE), pl.ds(c + LANES, BLOCK_COLS)]
    tall = BLOCK_ROWS + 2 * EDGE
    slope_y = pltpu.roll(down, tall - 1, 0) - pltpu.roll(down, 1, 0)
    slope_y = slope_y[EDGE : EDGE + BLOCK_ROWS, :]
    return value, slope_x, slope_y


def fold(array):
    rows, cols = array.shape
    out = jnp.zeros((8, LANES), jnp.float32)
    for a in range(rows // 8):
        for b in range(cols // LANES):
            out = out + array[a * 8 : a * 8 + 8, b * LANES : b * LANES + LANES]
    return out


def warp_kernel(above_ref, m_ref, below_ref, edges_ref, mixed_ref, flat_ref, acc_ref, out_ref, acc_out, wide):
    acc_out[...] = acc_ref[...]
    step, rows, cols = pl.program_id(0), m_ref.shape[0], m_ref.shape[1]
    zeros = jnp.zeros((rows + 2 * EDGE, LANES), jnp.float32)
    wide[:, pl.ds(0, LANES)] = zeros
    wide[:, pl.ds(cols + LANES, LANES)] = zeros
    above = above_ref[...].astype(jnp.float32)[EDGE:]
    below = below_ref[...].astype(jnp.float32)[:EDGE]
    inner = pl.ds(LANES, cols)
    wide[pl.ds(0, EDGE), inner] = jnp.where(step == 0, edges_ref[pl.ds(0, EDGE), :], above)
    wide[pl.ds(EDGE + rows, EDGE), inner] = jnp.where(
        step == pl.num_programs(0) - 1, edges_ref[pl.ds(EDGE, EDGE), :], below
    )
    wide[pl.ds(EDGE, rows), inner] = m_ref[...].astype(jnp.float32)

    @pl.loop(0, cols // BLOCK_COLS, unroll=2)
    def _(j):
        c = pl.multiple_of(j * BLOCK_COLS, BLOCK_COLS)
        value, sx, sy = slopes_of(wide, 0, c)
        flat = flat_ref[:, pl.ds(c, BLOCK_COLS)]
        shift_x = jnp.dot(mixed_ref[:, :GRID_SIZE], flat, preferred_element_type=jnp.float32)
        shift_y = jnp.dot(mixed_ref[:, GRID_SIZE:], flat, preferred_element_type=jnp.float32)
        out_ref[:, pl.ds(c, BLOCK_COLS)] = (value + shift_x * sx + shift_y * sy).astype(jnp.bfloat16)


def warp(moving, edges, mixed, flat, accumulated):
    rows, cols = moving.shape
    thin = 2 * EDGE
    ratio, last = BLOCK_ROWS // thin, rows // thin - 1
    whole = lambda shape: pl.BlockSpec(shape, lambda i: (0, 0))
    return pl.pallas_call(
        warp_kernel,
        grid=(rows // BLOCK_ROWS,),
        out_shape=(
            jax.ShapeDtypeStruct((rows, cols), jnp.bfloat16),
            jax.ShapeDtypeStruct(accumulated.shape, jnp.float32),
        ),
        in_specs=[
            pl.BlockSpec((thin, cols), lambda i: (jnp.maximum(ratio * i - 1, 0), 0)),
            pl.BlockSpec((BLOCK_ROWS, cols), lambda i: (i, 0)),
            pl.BlockSpec((thin, cols), lambda i: (jnp.minimum(ratio * i + ratio, last), 0)),
            whole(edges.shape),
            pl.BlockSpec((BLOCK_ROWS, LANES), lambda i: (i, 0)),
            whole(flat.shape),
            whole(accumulated.shape),
        ],
        out_specs=(pl.BlockSpec((BLOCK_ROWS, cols), lambda i: (i, 0)), whole(accumulated.shape)),
        scratch_shapes=[pltpu.VMEM((BLOCK_ROWS + 2 * EDGE, cols + 2 * LANES), jnp.float32)],
        compiler_params=pltpu.CompilerParams(vmem_limit_bytes=VMEM_BYTES),
    )(moving, moving, moving, edges, mixed, flat, accumulated)


MESH = pl.DeviceIdType.MESH
HEAD = 8
HALO = 16
FIELDS = 7
SPAN = 1024
F32 = jnp.float32
BF16 = jnp.bfloat16


def window_of(knots):
    return 16 + max(8, -(-knots // 8) * 8)


def narrow_of(knots):
    return -(-(knots + 8) // 8) * 8


def base_of(strip, knots):
    return lax.div(strip * knots, 8) * 8


def flat_table(cols):
    pixels = np.arange(cols, dtype=np.float32)[None, :]
    knots = np.arange(GRID_SIZE, dtype=np.float32)[:, None]
    offset = (pixels + np.float32(0.5)) / np.float32(cols // GRID_SIZE) - knots - np.float32(0.5)
    distance = np.abs(offset)
    near = np.float32(2.0 / 3.0) - distance * distance + np.float32(0.5) * distance * distance * distance
    remain = np.float32(2.0) - distance
    far = remain * remain * remain / np.float32(6.0)
    return np.where(distance < 1, near, np.where(distance < 2, far, np.float32(0))).astype(BF16)


def strip_basis(shape, pixel_dim, first_row, first_knot, spacing):
    pixels = (first_row + lax.broadcasted_iota(jnp.int32, shape, pixel_dim)).astype(F32)
    knot_pos = (first_knot + lax.broadcasted_iota(jnp.int32, shape, 1 - pixel_dim)).astype(F32)
    return spline_weight((pixels + 0.5) * (1.0 / spacing) - knot_pos - 0.5)


def column_tables(basis_ref, pairs_ref, spacing):
    middle = GRID_SIZE // 2
    wide = BAND * GRID_SIZE
    shape = (spacing, wide)
    lane = lax.broadcasted_iota(jnp.int32, shape, 1)
    pixel = (middle * spacing + lax.broadcasted_iota(jnp.int32, shape, 0)).astype(F32)
    place = (pixel + 0.5) * (1.0 / spacing) - 0.5
    knot, band = lax.rem(lane, GRID_SIZE), lax.div(lane, GRID_SIZE)
    rounded = lambda values: values.astype(BF16).astype(F32)
    single = rounded(spline_weight(place - knot.astype(F32)))
    product = single * rounded(spline_weight(place - (knot + band).astype(F32)))
    one_lane = lax.broadcasted_iota(jnp.int32, (spacing, LANES), 1)
    one_knot = lax.rem(one_lane, GRID_SIZE)

    @pl.loop(0, GRID_SIZE)
    def _(t):
        at = pl.ds(pl.multiple_of(t * spacing, spacing), spacing)
        shift = lax.rem(t - middle + LANES, LANES)
        close = jnp.abs(one_knot - t) <= BAND
        moved = jnp.where(close, pltpu.roll(single[:, :LANES], shift, 1), 0.0)
        for k in range(2):
            half = one_lane < GRID_SIZE if k == 0 else one_lane >= GRID_SIZE
            basis_ref[k, at, :] = jnp.where(half, moved, 0.0).astype(BF16)
        for k in range(wide // LANES):
            cols = slice(k * LANES, (k + 1) * LANES)
            reach = one_knot + (k * LANES // GRID_SIZE + lax.div(one_lane, GRID_SIZE))
            keep = close & (reach < GRID_SIZE)
            rolled = jnp.where(keep, pltpu.roll(product[:, cols], shift, 1), 0.0)
            pairs_ref[at, cols] = rolled.astype(BF16)


def fill_rows(wide, at, source, row, count, skip=0):
    cols = source.shape[1]
    values = source[pl.ds(row, count + skip), :].astype(F32)
    wide[pl.ds(at, count), pl.ds(LANES, cols)] = values[skip:]


def fill_body(wide, source, offset, rows):
    @pl.loop(0, rows // BLOCK_ROWS)
    def _(i):
        r = pl.multiple_of(i * BLOCK_ROWS, BLOCK_ROWS)
        fill_rows(wide, EDGE + r, source, pl.multiple_of(offset + r, 16), BLOCK_ROWS)


def blocks(rows, start, body):
    per_row = SPAN // BLOCK_COLS

    @pl.loop(0, rows // BLOCK_ROWS * per_row)
    def _(step):
        i, j = lax.div(step, per_row), lax.rem(step, per_row)
        r = pl.multiple_of(i * BLOCK_ROWS, BLOCK_ROWS)
        c = pl.multiple_of(j * BLOCK_COLS, BLOCK_COLS)
        body(r, c, pl.multiple_of(start + c, BLOCK_COLS))


def still_tables(wide, fields, basis_ref, pairs_ref, lin, raw, sums, rows, cols):
    dot = functools.partial(jnp.dot, preferred_element_type=F32)

    @pl.loop(0, cols // SPAN)
    def _(part):
        start = pl.multiple_of(part * SPAN, SPAN)

        def body(r, c, at):
            value, sx, sy = slopes_of(wide, r, at)
            here = (pl.ds(r, BLOCK_ROWS), pl.ds(c, BLOCK_COLS))
            for k, field in enumerate((value * sx, value * sy, sx, sy, sx * sx, sx * sy, sy * sy)):
                fields[(k, *here)] = field.astype(BF16)
            sums[1] += fold(value)
            sums[3] += fold(value * value)

        blocks(rows, start, body)
        cut = pl.ds(start, SPAN)
        for k in range(2):
            lin[1 + k] += dot(fields[2 * k], basis_ref[0, cut, :]) + dot(fields[2 * k + 1], basis_ref[1, cut, :])
        for k in range(3):
            raw[k] += dot(fields[4 + k], pairs_ref[cut, :])


def rest_tables(wide, fixed, fixed_row, fields, basis_ref, lin, sums, rows, cols, target=0):
    dot = functools.partial(jnp.dot, preferred_element_type=F32)

    @pl.loop(0, cols // SPAN)
    def _(part):
        start = pl.multiple_of(part * SPAN, SPAN)

        def body(r, c, at):
            value, sx, sy = slopes_of(wide, r, at)
            f = fixed[pl.ds(pl.multiple_of(fixed_row + r, BLOCK_ROWS), BLOCK_ROWS), pl.ds(at, BLOCK_COLS)]
            f = f.astype(F32)
            rest = f - value
            here = (pl.ds(r, BLOCK_ROWS), pl.ds(c, BLOCK_COLS))
            fields[(0, *here)] = (rest * sx).astype(BF16)
            fields[(1, *here)] = (rest * sy).astype(BF16)
            sums[0] += fold(f)
            sums[2] += fold(rest * value)

        blocks(rows, start, body)
        cut = pl.ds(start, SPAN)
        here = pl.ds(0, rows)
        lin[0, pl.ds(target, rows)] += dot(fields[0, here], basis_ref[0, cut, :]) + dot(
            fields[1, here], basis_ref[1, cut, :]
        )


def quad_tables(raw, quad):
    for d in range(BAND):
        at = slice(d * GRID_SIZE, (d + 1) * GRID_SIZE)
        xx, xy, yy = (0.25 * raw[k, :, at] for k in range(3))
        quad[d] = jnp.concatenate([xx, yy], axis=1)
        quad[BAND + d] = jnp.concatenate([xy, xy], axis=1)


def head_rows(sums, keys):
    zero = jnp.zeros((1, LANES), F32)
    rows = [jnp.sum(sums[k], axis=0, keepdims=True) if k in keys else zero for k in range(4)]
    return jnp.concatenate(rows + [jnp.zeros((HEAD - 4, LANES), F32)], axis=0)


def thirds(values):
    high = values.astype(BF16).astype(F32)
    rest = values - high
    middle = rest.astype(BF16).astype(F32)
    return high, middle, (rest - middle).astype(BF16).astype(F32)


def mix(row_six, control):
    high, middle, low = thirds(control)
    six = jnp.concatenate([high, middle, high, low, middle, high], axis=0).astype(BF16)
    return jnp.dot(row_six[...], six, preferred_element_type=F32)


def project_rows(row_three, values):
    window = row_three.shape[0] // 3
    out = 0.0
    for k, part in enumerate(thirds(values)):
        product = jnp.dot(row_three[...], part.astype(BF16), preferred_element_type=F32)
        for j in range(3 - k):
            out += product[j * window : (j + 1) * window]
    return out


def grand(values):
    return jnp.sum(jnp.sum(values, axis=0, keepdims=True), axis=1, keepdims=True)


def track_kernel(strips, chain, m_ref, anchor_ref, acc_ref, mixed_ref, edges_ref, *scratch):
    (fixed, low, top, bottom, tail, first_row, last_row, wide, low_wide, fields, basis_ref, pairs_ref, lin, raw, quad, sums) = scratch[:16]
    (row_six, row_three, moved, hist, parts, side, near, ends, grads) = scratch[16:25]
    (quad_send, quad_recv, side_send, side_recv, near_send, near_recv) = scratch[25:31]
    (end_send, end_recv, bulk_send, bulk_recv, local_sem) = scratch[31:]
    rows, cols = m_ref.shape
    half = rows // 2
    me, link = lax.axis_index("quad"), lax.axis_index("chain")
    knots = GRID_SIZE // strips
    window, narrow = window_of(knots), narrow_of(knots)
    early = ITERATIONS + 1
    spacing = rows * strips // GRID_SIZE
    pixel_count = float(rows * strips * cols)
    base = base_of(me, knots)
    first, last = link == 0, link == chain - 1
    steps = range(1, strips)

    def mesh_copy(src, dst, send, recv, to):
        return pltpu.make_async_remote_copy(
            src_ref=src, dst_ref=dst, send_sem=send, recv_sem=recv, device_id=to, device_id_type=MESH
        )

    barrier = pltpu.get_barrier_semaphore()

    def greet(to):
        pl.semaphore_signal(barrier, inc=1, device_id=to, device_id_type=MESH)

    for step in steps:
        greet({"quad": lax.rem(me + step, strips)})
    for step in range(1, chain):
        greet({"chain": lax.rem(link + step, chain)})
    for edge, to in ((last, link + 1), (first, link - 1)):

        @pl.when(jnp.logical_not(edge))
        def _():
            for step in steps:
                greet({"chain": to, "quad": lax.rem(me + step, strips)})

    load_anchor = pltpu.make_async_copy(anchor_ref, fixed, local_sem)

    @pl.when(first)
    def _():
        load_anchor.start()

    first_row[...] = m_ref[pl.ds(0, HALO), :].astype(F32)[:1]
    last_row[...] = m_ref[pl.ds(rows - HALO, HALO), :].astype(F32)[HALO - 1 :]
    begin = me * rows
    lane = lax.broadcasted_iota(jnp.int32, (rows, 6 * window), 1)
    group = sum((lane >= k * window).astype(jnp.int32) for k in range(1, 6))
    pixels = (begin + lax.broadcasted_iota(jnp.int32, (rows, 6 * window), 0)).astype(F32)
    knot_pos = (base - 8 + lane - window * group).astype(F32)
    high, middle, small = thirds(spline_weight((pixels + 0.5) * (1.0 / spacing) - knot_pos - 0.5))
    is_middle = (group == 2) | (group == 4)
    row_six[...] = jnp.where(group == 5, small, jnp.where(is_middle, middle, high)).astype(BF16)
    rows_t = thirds(strip_basis((narrow, rows), 1, begin, me * knots - 4, spacing))
    row_three[...] = jnp.concatenate(rows_t, axis=0).astype(BF16)
    fill_body(wide, m_ref, 0, rows)
    cross = jnp.where(first, 0, strips - 1) + jnp.where(last, 0, strips - 1)
    pl.semaphore_wait(barrier, strips - 1 + chain - 1 + cross)

    to_top = mesh_copy(last_row, top, bulk_send.at[0], bulk_recv.at[0], {"quad": me + 1})
    to_bottom = mesh_copy(first_row, bottom, bulk_send.at[1], bulk_recv.at[1], {"quad": me - 1})
    def up(count):
        at = pl.ds(0, count)
        return mesh_copy(m_ref.at[at], fixed.at[at], bulk_send.at[2], bulk_recv.at[2], {"chain": link + 1})

    def down(count):
        source = m_ref.at[pl.ds(rows - count - HALO, count + HALO)]
        target = low.at[pl.ds(half - count, count + HALO)]
        return mesh_copy(source, target, bulk_send.at[3], bulk_recv.at[3], {"chain": link - 1})

    across = mesh_copy(
        first_row,
        tail,
        bulk_send.at[4],
        bulk_recv.at[4],
        {"chain": link - 1, "quad": me - 1},
    )
    inner_top, inner_bottom = me > 0, me < strips - 1
    later, earlier = jnp.logical_not(last), jnp.logical_not(first)
    even = lax.rem(link, 2) == 0
    odd = jnp.logical_not(even)
    wide_share = 3 * rows // 4
    pl.when(inner_bottom)(lambda: to_top.start())
    pl.when(inner_top)(lambda: to_bottom.start())
    pl.when(later & even)(lambda: up(wide_share).start())
    pl.when(later & odd)(lambda: up(half).start())
    pl.when(earlier & odd)(lambda: down(rows - wide_share).start())
    pl.when(earlier & even)(lambda: down(half).start())
    pl.when(jnp.logical_and(earlier, inner_top))(lambda: across.start())

    @pl.when(me == 0)
    def _():
        top[...] = jnp.zeros_like(top)

    @pl.when(me == strips - 1)
    def _():
        bottom[...] = jnp.zeros_like(bottom)
        tail[...] = jnp.zeros_like(tail)

    @pl.when(first)
    def _():
        near[:, 0] = jnp.zeros_like(near[:, 0])
        side[...] = jnp.zeros_like(side)

    @pl.when(last)
    def _():
        near[:, 1] = jnp.zeros_like(near[:, 1])

    for ref in (hist, grads, lin, raw, sums):
        ref[...] = jnp.zeros_like(ref)
    zeros = jnp.zeros((rows + 2 * EDGE, LANES), F32)
    for at in (0, cols + LANES):
        wide[:, pl.ds(at, LANES)] = zeros
        low_wide[:, pl.ds(at, LANES)] = zeros[: half + 2 * EDGE]
    column_tables(basis_ref, pairs_ref, cols // GRID_SIZE)
    pl.when(inner_top)(lambda: to_top.wait_recv())
    pl.when(inner_bottom)(lambda: to_bottom.wait_recv())
    for k, row in enumerate((top, bottom)):
        values = jnp.broadcast_to(row[...], (EDGE, cols))
        edges_ref[pl.ds(k * EDGE, EDGE), :] = values
        wide[pl.ds(k * (EDGE + rows), EDGE), pl.ds(LANES, cols)] = values

    still_tables(wide, fields, basis_ref, pairs_ref, lin, raw, sums, rows, cols)
    quad_tables(raw, quad)

    def spread(turn, count):
        copies = []
        for step in steps:
            at = parts.at[turn, me, pl.ds(0, count)]
            to = {"quad": lax.rem(me + step, strips)}
            copies.append(mesh_copy(at, at, quad_send.at[turn, step], quad_recv.at[turn, me], to))
        for copy in copies:
            copy.start()
        return copies

    def gathered(turn, count):
        for step in steps:
            peer = lax.rem(me + step, strips)
            at = parts.at[turn, peer, pl.ds(0, count)]
            mesh_copy(at, at, quad_send.at[turn, step], quad_recv.at[turn, peer], {"quad": peer}).wait_recv()

    def side_copy(row, step):
        to = {"chain": link + 1, "quad": lax.rem(me + step, strips)}
        return mesh_copy(parts.at[ITERATIONS, me, pl.ds(0, HEAD + narrow)], side.at[row], side_send.at[step], side_recv.at[row], to)

    still_sums = (1, 3)

    def own_part(wait, count):
        wait()
        sums[...] = jnp.zeros_like(sums)
        rest_tables(wide, fixed, 0, fields, basis_ref, lin, sums, count, cols)
        parts[0, me, pl.ds(HEAD, narrow)] = 0.5 * project_rows(row_three, lin[0])
        parts[0, me, pl.ds(0, HEAD)] = head_rows(sums, (0, 2))

    def later_part(count):
        down(count).wait_recv()
        pl.when(inner_bottom)(lambda: across.wait_recv())
        fill_body(low_wide, low, HALO + half - count, count)
        begin_low = half - count
        fill_rows(low_wide, 0, low, begin_low, EDGE, EDGE)
        low_wide[pl.ds(EDGE + count, EDGE), pl.ds(LANES, cols)] = jnp.broadcast_to(tail[...], (EDGE, cols))
        sums[...] = jnp.zeros_like(sums)
        lin[1] = jnp.zeros_like(lin[1])
        rest_tables(low_wide, m_ref, rows - count, fields, basis_ref, lin.at[pl.ds(1, 1)], sums, count, cols, rows - count)
        parts[ITERATIONS, me, pl.ds(0, HEAD)] = head_rows(sums, (0, 2))
        parts[ITERATIONS, me, pl.ds(HEAD, narrow)] = 0.5 * project_rows(row_three, lin[1])
        for step in range(strips):
            side_copy(me, step).start()

    parts[early, me, pl.ds(0, HEAD)] = head_rows(sums, still_sums)
    for k in range(2):
        parts[early, me, pl.ds(HEAD + k * narrow, narrow)] = 0.5 * project_rows(row_three, lin[1 + k])
    sends = spread(early, HEAD + 2 * narrow)
    pl.when(even & later)(lambda: later_part(rows - wide_share))
    pl.when(first)(lambda: own_part(load_anchor.wait, rows))
    pl.when(even & earlier)(lambda: own_part(up(half).wait_recv, half))
    pl.when(odd)(lambda: own_part(up(wide_share).wait_recv, wide_share))
    sends += spread(0, HEAD + narrow)
    pl.when(odd & later)(lambda: later_part(half))
    gathered(early, HEAD + 2 * narrow)
    gathered(0, HEAD + narrow)

    @pl.when(earlier)
    def _():
        for step in range(strips):
            side_copy(lax.rem(me + step, strips), step).wait_recv()

    def near_copy(turn, side_of):
        to = {"chain": link + 1 if side_of == 0 else link - 1}
        src = hist.at[turn, pl.ds(8, GRID_SIZE)]
        return mesh_copy(src, near.at[turn, side_of], near_send.at[turn, side_of], near_recv.at[turn, side_of], to)

    def collect(ref, turn, offset, slot):
        for strip in range(strips):
            here = (strip, pl.ds(offset, narrow))
            grads[slot, pl.ds(strip * knots + 4, narrow)] += ref[here] if turn is None else ref[(turn, *here)]
        return grads[slot, pl.ds(8, GRID_SIZE)]

    at = pl.ds(0, HEAD)
    head = 0.0
    for strip in range(strips):
        head = head + (parts[0, strip, at] + parts[early, strip, at] + side[strip, at])
    head = jnp.sum(head, axis=1, keepdims=True)
    total = [head[k : k + 1, :] for k in range(4)]
    collect(side, None, HEAD, 0)
    grad_rest = collect(parts, 0, HEAD, 0)
    grad_still, grad_ones = (collect(parts, early, HEAD + k * narrow, 1 + k) for k in range(2))
    fixed_mean = total[0] / pixel_count
    block = 128

    for turn in range(ITERATIONS):
        moving_sum, moving_sq, cross_sum = total[1], total[3], total[2] + total[3]
        grad_extra = 0.0
        before = hist[turn, pl.ds(8, GRID_SIZE)]
        smooth = 0.0
        if turn:
            mixed_all = mix(row_six, hist[turn, pl.ds(base, window)])
            moved[...] = mixed_all.astype(BF16).astype(F32)

            @pl.loop(0, rows // block)
            def _(i):
                r = pl.ds(pl.multiple_of(i * block, block), block)
                mixed = moved[r, :]
                other = pltpu.roll(mixed, GRID_SIZE, 1)
                out = quad[0, r, :] * mixed + quad[BAND, r, :] * other
                for d in range(1, BAND):
                    q, p = quad[d, r, :], quad[BAND + d, r, :]
                    out += q * pltpu.roll(mixed, LANES - d, 1) + p * pltpu.roll(other, LANES - d, 1)
                    out += pltpu.roll(q * mixed + p * other, d, 1)
                moved[r, :] = out

            parts[turn, me, pl.ds(0, narrow)] = project_rows(row_three, moved[...])
            sends += spread(turn, narrow)
            gathered(turn, narrow)
            grad_extra = collect(parts, turn, 0, 2 + turn)
            moving_sum = moving_sum + grand(before * grad_ones)
            moving_sq = moving_sq + grand(before * (2.0 * grad_still + grad_extra))
            cross_sum = cross_sum + grand(before * (grad_rest + grad_still))
            pl.when(earlier)(lambda: near_copy(turn, 0).wait_recv())
            pl.when(later)(lambda: near_copy(turn, 1).wait_recv())
            smooth = near[turn, 0] - 2.0 * before + near[turn, 1]
        moving_mean = moving_sum / pixel_count
        moving_var = moving_sq - pixel_count * moving_mean * moving_mean
        cross_var = cross_sum - pixel_count * fixed_mean * moving_mean
        denominator = jnp.sqrt(moving_var + EPSILON)
        ratio = cross_var / denominator / (moving_var + EPSILON)
        gradient = pixel_count * (
            (grad_rest + grad_still - fixed_mean * grad_ones) / denominator
            - ratio * (grad_still + grad_extra - moving_mean * grad_ones)
        )
        size = grand(gradient * gradient) / (2.0 * GRID_SIZE * GRID_SIZE)
        direction = gradient / jnp.sqrt(size + EPSILON)
        hist[turn + 1, pl.ds(8, GRID_SIZE)] = before + direction / ITERATIONS + SMOOTHING * smooth
        if turn < ITERATIONS - 1:
            pl.when(later)(lambda: near_copy(turn + 1, 0).start())
            pl.when(earlier)(lambda: near_copy(turn + 1, 1).start())

    def end_copy(owner, step):
        src = hist.at[ITERATIONS, pl.ds(8, GRID_SIZE)]
        to = {"chain": lax.rem(link + step, chain)}
        return mesh_copy(src, ends.at[owner], end_send.at[step], end_recv.at[owner], to)

    for step in range(1, chain):
        end_copy(link, step).start()
    ends[link] = hist[ITERATIONS, pl.ds(8, GRID_SIZE)]
    for step in range(1, chain):
        end_copy(lax.rem(link + step, chain), step).wait_recv()
    out = ends[0]
    for owner in range(1, chain):
        out = out + jnp.where(owner <= link, ends[owner], 0.0)
    acc_ref[...] = out
    hist[0, pl.ds(8, GRID_SIZE)] = out
    mixed_ref[...] = mix(row_six, hist[0, pl.ds(base, window)]).astype(BF16) * jnp.asarray(0.5, BF16)
    for copy in sends:
        copy.wait_send()
    for turn in range(1, ITERATIONS):
        pl.when(later)(lambda: near_copy(turn, 0).wait_send())
        pl.when(earlier)(lambda: near_copy(turn, 1).wait_send())
    for step in range(1, chain):
        end_copy(link, step).wait_send()
    pl.when(inner_bottom)(lambda: to_top.wait_send())
    pl.when(inner_top)(lambda: to_bottom.wait_send())
    pl.when(earlier & odd)(lambda: down(rows - wide_share).wait_send())
    pl.when(earlier & even)(lambda: down(half).wait_send())
    pl.when(later & even)(lambda: up(wide_share).wait_send())
    pl.when(later & odd)(lambda: up(half).wait_send())
    pl.when(jnp.logical_and(earlier, inner_top))(lambda: across.wait_send())

    @pl.when(later)
    def _():
        for step in range(strips):
            side_copy(me, step).wait_send()


def track(moving, anchor):
    rows, cols = moving.shape
    strips, chain = lax.axis_size("quad"), lax.axis_size("chain")
    window = window_of(GRID_SIZE // strips)
    vmem = pl.BlockSpec(memory_space=pltpu.VMEM)
    tall = GRID_SIZE + 16 + window
    dma = pltpu.SemaphoreType.DMA
    return pl.pallas_call(
        functools.partial(track_kernel, strips, chain),
        out_shape=(
            jax.ShapeDtypeStruct((GRID_SIZE, LANES), F32),
            jax.ShapeDtypeStruct((rows, LANES), BF16),
            jax.ShapeDtypeStruct((2 * EDGE, cols), F32),
        ),
        in_specs=[vmem, pl.BlockSpec(memory_space=pl.ANY)],
        out_specs=[vmem] * 3,
        scratch_shapes=[
            pltpu.VMEM((rows, cols), BF16),
            pltpu.VMEM((rows // 2 + HALO, cols), BF16),
        ]
        + [pltpu.VMEM((1, cols), F32)] * 5
        + [
            pltpu.VMEM((rows + 2 * EDGE, cols + 2 * LANES), F32),
            pltpu.VMEM((rows // 2 + 2 * EDGE, cols + 2 * LANES), F32),
            pltpu.VMEM((FIELDS, rows, SPAN), BF16),
            pltpu.VMEM((2, cols, LANES), BF16),
            pltpu.VMEM((cols, BAND * GRID_SIZE), BF16),
            pltpu.VMEM((3, rows, LANES), F32),
            pltpu.VMEM((3, rows, BAND * GRID_SIZE), F32),
            pltpu.VMEM((2 * BAND, rows, LANES), F32),
            pltpu.VMEM((4, 8, LANES), F32),
            pltpu.VMEM((rows, 6 * window), BF16),
            pltpu.VMEM((3 * narrow_of(GRID_SIZE // strips), rows), BF16),
            pltpu.VMEM((rows, LANES), F32),
            pltpu.VMEM((ITERATIONS + 1, tall, LANES), F32),
            pltpu.VMEM((ITERATIONS + 2, strips, HEAD + 2 * narrow_of(GRID_SIZE // strips), LANES), F32),
            pltpu.VMEM((strips, HEAD + narrow_of(GRID_SIZE // strips), LANES), F32),
            pltpu.VMEM((ITERATIONS + 1, 2, GRID_SIZE, LANES), F32),
            pltpu.VMEM((chain, GRID_SIZE, LANES), F32),
            pltpu.VMEM((ITERATIONS + 2, tall, LANES), F32),
            dma((ITERATIONS + 2, strips)),
            dma((ITERATIONS + 2, strips)),
            dma((strips,)),
            dma((strips,)),
            dma((ITERATIONS + 1, 2)),
            dma((ITERATIONS + 1, 2)),
            dma((chain,)),
            dma((chain,)),
            dma((5,)),
            dma((5,)),
            dma,
        ],
        compiler_params=pltpu.CompilerParams(
            collective_id=0, has_side_effects=True, vmem_limit_bytes=VMEM_BYTES
        ),
    )(moving, anchor)


def local(sections, anchor):
    moving = sections[0]
    accumulated, mixed, edges = track(moving, anchor)
    registered, accumulated = warp(moving, edges, mixed, flat_table(moving.shape[1]), accumulated)
    return registered[None], accumulated[None]


def solution(mesh):
    in_specs = (P("chain", "quad", None), P("quad", None))
    out_specs = (P("chain", "quad", None), P("chain", None, None))
    return jax.shard_map(local, mesh=mesh, in_specs=in_specs, out_specs=out_specs, check_vma=False)
```
